32 devices in a mesh: groups: 2 (over y), space: 4 (over z), mp: 2 (over x), sub: 2 (over core).
Axes of the slice: x: 2, y: 2, z: 4, core: 2. Of those that a mesh axis runs over, the one named last changes fastest.
Arguments:
- voxels: bfloat16 [24576, 512], P(('groups', 'space', 'sub')), parts along dimension 0, may hold values from -6 to 6
- window_ids: int32 [24576], P(('groups', 'space', 'sub')), parts along dimension 0, may hold values from 0 to 127, as said below
- voxel_slots: int32 [24576], P(('groups', 'space', 'sub')), parts along dimension 0, may hold values from 0 to 255, as said below
- window_counts: int32 [256], P('groups'), parts along dimension 0, may hold values from 0 to 256, as said below
- norm_gain: float32 [512], replicated, may hold values from 0.25 to 1.75
- w_query_key: bfloat16 [2, 512, 512], P(None, None, 'mp'), may hold values from -2 to 2
- w_value: bfloat16 [512, 512], P(None, 'mp'), may hold values from -0.25 to 0.25
- w_out: bfloat16 [512, 512], P('mp'), may hold values from -0.25 to 0.25
- ffn_gain: float32 [512], replicated, may hold values from 0.25 to 1.75
- w_up: bfloat16 [512, 2048], P(None, 'mp'), may hold values from -0.25 to 0.25
- w_down: bfloat16 [2048, 512], P('mp'), may hold values from -0.125 to 0.125
Outputs:
- result: bfloat16 [24576, 512], P(('groups', 'space', 'sub'), 'mp'), parts along dimension 0
The draws below stay inside these ranges and needn't reach their ends.
There are 2 independent parts, one for each index of `groups`. The reference program is written for one: setup_inputs(seed, part) draws one part's arguments, and reference() takes and returns one part's arrays. A program takes and returns all parts, laid end to end along the dimension named above; an argument that names none is the same for every part. Nothing has to cross between parts.
Inputs may be any that keep to these rules, and one draw needn't show every extreme that they name: `window_ids`: window w belongs to owner w // 16 (its index along space+sub) as that owner's window w % 16. On the voxels of one device at most 384 lie in windows of one owner, and in every draw some owner has exactly 384 voxels of every device. `voxel_slots`: the voxels of a window hold slots 0 to its count - 1, each once. window_counts[w] is the number of voxels with window id w; some window holds 256.
All inputs are finite; a program needn't handle non-finite values.
Results may differ from the reference program's by a relative error of at most 0.012.
Values may be sent and summed in bfloat16 or wider, within the bound.
No kernel may reach another device: no remote copies, remote signals or barrier semaphores. Data moves between devices by JAX's collectives and lax.ppermute only.
A program may use at most 128 MiB of HBM per device.

```python
import jax
import jax.numpy as jnp
from jax import lax

D = 512
HEADS = 8
HDIM = 64
FF = 2048
WLEN = 256
VOX_DEV = 1536
NOWN = 8
VOX = 12288
CAP = 384
WIN_DEV = 16
NWIN = 128


def scene(key):
    owner_total = NOWN
    capacity = CAP
    per_owner = WIN_DEV
    key_bias = jax.random.fold_in(key, 101)
    key_first = jax.random.fold_in(key, 102)
    key_score = jax.random.fold_in(key, 103)
    key_shuffle = jax.random.fold_in(key, 104)
    key_sizes = jax.random.fold_in(key, 105)
    bias = jax.random.randint(key_bias, (owner_total,), 0, 3)
    busiest = jax.random.randint(key_first, (), 0, owner_total)
    bias = jnp.where(jnp.arange(owner_total) == busiest, 3, bias)
    scores = jax.random.randint(key_score, (owner_total, owner_total, capacity), 0, 1 << 20) + (bias * (1 << 20))[None, :, None]
    scores = scores.reshape(owner_total, owner_total * capacity)
    chosen = jnp.argsort(-scores, axis=1, stable=True)[:, :VOX_DEV].astype(jnp.int32)
    source_ids = jnp.arange(owner_total, dtype=jnp.int32)[:, None]
    selected = jnp.zeros((owner_total, owner_total * capacity), jnp.int32).at[source_ids, chosen].set(1)
    shuffles = jax.vmap(lambda sub_key: jax.random.permutation(sub_key, VOX_DEV))(jax.random.split(key_shuffle, owner_total))
    slot_ids = jnp.take_along_axis(chosen, shuffles.astype(jnp.int32), axis=1)
    owner_of = slot_ids // capacity
    column_of = slot_ids % capacity
    by_owner = selected.reshape(owner_total, owner_total, capacity).transpose(1, 0, 2).reshape(owner_total, owner_total * capacity)
    earlier = (jnp.cumsum(by_owner, axis=1) - by_owner).reshape(owner_total, owner_total, capacity)
    rank_of = earlier[owner_of, jnp.broadcast_to(source_ids, owner_of.shape), column_of]
    sizes = jax.random.randint(key_sizes, (owner_total, per_owner), 3 * WLEN // 4, WLEN + 1)
    sizes = sizes.at[:, 0].set(WLEN)
    ends = jnp.cumsum(sizes, axis=1)
    starts = ends - sizes
    local_win = jnp.sum((rank_of[:, :, None] >= ends[owner_of]).astype(jnp.int32), axis=-1)
    slot_in = rank_of - jnp.take_along_axis(starts[owner_of], local_win[:, :, None], axis=-1)[:, :, 0]
    load = jnp.sum(selected.reshape(owner_total, owner_total, capacity), axis=(0, 2))
    counts_flat = jnp.clip(load[:, None] - starts, 0, sizes).reshape(-1)
    window_of = owner_of * per_owner + local_win
    return (window_of.reshape(-1).astype(jnp.int32), slot_in.reshape(-1).astype(jnp.int32), counts_flat.astype(jnp.int32))


def draw_window_ids(key, part):
    return scene(key)[0]


def draw_voxel_slots(key, part):
    return scene(key)[1]


def draw_window_counts(key, part):
    return scene(key)[2]


def draw_w_query_key(key, part):
    key_base = jax.random.fold_in(key, 201)
    stacked = jax.random.normal(key_base, (2, D, D), jnp.float32) * D ** (-0.5)
    return jnp.clip(stacked, -2.0, 2.0).astype(jnp.bfloat16)


def block_scale(rng, dims, pieces, low, high):
    factor_of, own = 1.0, jax.random.fold_in(rng, 6)
    for axis_at, shards_of in pieces:
        heights = jnp.exp(jax.random.uniform(jax.random.fold_in(own, axis_at), (shards_of,), jnp.float32, low / len(pieces), high / len(pieces)))
        factor_of = factor_of * jnp.repeat(heights, dims[axis_at] // shards_of).reshape([-1 if axis == axis_at else 1 for axis in range(len(dims))])
    return factor_of


def scatter_about(stream_key, dims, deviation, limit, pieces=(), kind=jnp.bfloat16):
    values = jax.random.normal(stream_key, dims, jnp.float32) * deviation
    if len(pieces) > 0:
        values = block_scale(stream_key, dims, pieces, -0.22, 0.18) * values
    return jnp.clip(values, min=-limit, max=limit).astype(kind)


def setup_inputs(seed: int = 0, part: int = 0) -> dict:
    splits = jax.random.split(jax.random.key(seed), 12)
    part_splits = jax.random.split(jax.random.fold_in(splits[11], part), 12)
    voxels = scatter_about(part_splits[0], (VOX, D), 1.0, 6.0, ((0, 8),))
    window_ids = draw_window_ids(jax.random.fold_in(jax.random.fold_in(splits[11], part), 71), part)
    voxel_slots = draw_voxel_slots(jax.random.fold_in(jax.random.fold_in(splits[11], part), 71), part)
    window_counts = draw_window_counts(jax.random.fold_in(jax.random.fold_in(splits[11], part), 71), part)
    norm_gain = jnp.clip(1.0 + 0.15 * jax.random.normal(splits[4], (D,), jnp.float32), 0.25, 1.75)
    w_query_key = draw_w_query_key(jax.random.fold_in(splits[11], 71), part)
    w_value = scatter_about(splits[6], (D, D), D ** -0.5, 0.25, ((1, 2),))
    w_out = scatter_about(splits[7], (D, D), D ** -0.5, 0.25, ((0, 2),))
    ffn_gain = jnp.clip(1.0 + 0.15 * jax.random.normal(splits[8], (D,), jnp.float32), 0.25, 1.75)
    w_up = scatter_about(splits[9], (D, FF), D ** -0.5, 0.25, ((1, 2),))
    w_down = scatter_about(splits[10], (FF, D), FF ** -0.5, 0.125, ((0, 2),))
    return dict(voxels=voxels, window_ids=window_ids, voxel_slots=voxel_slots, window_counts=window_counts, norm_gain=norm_gain, w_query_key=w_query_key, w_value=w_value, w_out=w_out, ffn_gain=ffn_gain, w_up=w_up, w_down=w_down)


def normalize(values_in, gain):
    row_mean = lax.optimization_barrier(jnp.mean(values_in, axis=-1, keepdims=True))
    centred = values_in - row_mean
    variance = lax.optimization_barrier(jnp.mean(centred * centred, axis=-1, keepdims=True))
    return centred * lax.rsqrt(variance + 1e-05) * gain.astype(jnp.float32)

def reference(voxels, window_ids, voxel_slots, window_counts, norm_gain, w_query_key, w_value, w_out, ffn_gain, w_up, w_down):
    stream = voxels.astype(jnp.float32)
    normed = normalize(stream, norm_gain).astype(jnp.bfloat16)
    queries = jnp.dot(normed, w_query_key[0], preferred_element_type=jnp.float32).astype(jnp.bfloat16)
    key_rows = jnp.dot(normed, w_query_key[1], preferred_element_type=jnp.float32).astype(jnp.bfloat16)
    values = jnp.dot(normed, w_value, preferred_element_type=jnp.float32).astype(jnp.bfloat16)
    flat_index = (window_ids * WLEN + voxel_slots).astype(jnp.int32)
    slot_table = jnp.zeros((NWIN * WLEN,), jnp.int32).at[flat_index].set(jnp.arange(VOX, dtype=jnp.int32))
    slot_table = slot_table.reshape(NWIN, WLEN)

    def one_window(operands):
        members, count = operands
        split_shape = (WLEN, HEADS, HDIM)
        window_q = queries[members].astype(jnp.float32).reshape(split_shape)
        window_k = key_rows[members].astype(jnp.float32).reshape(split_shape)
        window_v = values[members].astype(jnp.float32).reshape(split_shape)
        scores = jnp.einsum('qhd,khd->hqk', window_q, window_k, precision=lax.Precision.HIGHEST) * HDIM ** (-0.5)
        live_keys = jnp.arange(WLEN, dtype=jnp.int32) < count
        scores = jnp.where(live_keys[None, None, :], scores, jnp.float32(-1e+30))
        row_max = lax.optimization_barrier(jnp.max(scores, axis=-1, keepdims=True))
        weights = jnp.exp(scores - row_max)
        probabilities = (weights / lax.optimization_barrier(jnp.sum(weights, axis=-1, keepdims=True))).astype(jnp.bfloat16)
        mixture = jnp.einsum('hqk,khd->qhd', probabilities.astype(jnp.float32), window_v, precision=lax.Precision.HIGHEST)
        return mixture.astype(jnp.bfloat16).reshape(WLEN, D)
    windows_out = lax.map(one_window, (slot_table, window_counts))
    attended = windows_out.reshape(NWIN * WLEN, D)[flat_index]
    after_attn = stream + jnp.dot(attended, w_out, preferred_element_type=jnp.float32)
    normed_ffn = normalize(after_attn, ffn_gain).astype(jnp.bfloat16)
    hidden = jax.nn.gelu(jnp.dot(normed_ffn, w_up, preferred_element_type=jnp.float32), approximate=True).astype(jnp.bfloat16)
    return (after_attn + jnp.dot(hidden, w_down, preferred_element_type=jnp.float32)).astype(jnp.bfloat16)
```

```python
import functools

import jax
import jax.numpy as jnp
from jax import lax
from jax.experimental import pallas as pl
from jax.experimental.pallas import tpu as pltpu
from jax.sharding import PartitionSpec as P

HDIM = 64
WLEN = 256
WIN_DEV = 16
META = 16
LANES = 128
OWN = ("space", "sub")


F32 = jnp.float32
BF16 = jnp.bfloat16
VM = pl.BlockSpec(memory_space=pltpu.VMEM)
PARAMS = pltpu.CompilerParams(vmem_limit_bytes=56 * 1024 * 1024)


class Steps:
    def __init__(self, n):
        self.n = n
        self.xor = n & (n - 1) == 0

    def to(self, i, k):
        return i ^ k if self.xor else (i + k) % self.n

    def frm(self, i, k):
        return i ^ k if self.xor else (i + self.n - k) % self.n

    def step(self, i, owner):
        return owner ^ i if self.xor else (owner + self.n - i) % self.n

    def perm(self, k, back=False):
        go = self.frm if back else self.to
        return [(i, go(i, k)) for i in range(self.n)]


def layer_norm(values_in, gain):
    row_mean = jnp.mean(values_in, axis=-1, keepdims=True)
    centred = values_in - row_mean
    variance = jnp.mean(centred * centred, axis=-1, keepdims=True)
    return centred * lax.rsqrt(variance + 1e-05) * gain


def dot(a, b):
    return jnp.dot(a, b, preferred_element_type=F32)


def own_index(sub_size):
    return lax.axis_index("space") * sub_size + lax.axis_index("sub")


def pack_kernel(ids_ref, vox_ref, gain_ref, *refs, steps, sub_size, near, cap, wins):
    n = steps.n
    col_ref, outs, normed_ref, cnt_ref = refs[0], refs[1 : 1 + n], refs[1 + n], refs[2 + n]
    rows, width = vox_ref.shape
    me = own_index(sub_size)
    mp = lax.axis_index("mp")
    normed_ref[...] = layer_norm(vox_ref[...].astype(F32), gain_ref[...]).astype(BF16)
    ids = ids_ref[...]
    step = 256
    win_iota = lax.broadcasted_iota(jnp.int32, (wins, step), 0)
    upper = (
        lax.broadcasted_iota(jnp.int32, (step, step), 0)
        < lax.broadcasted_iota(jnp.int32, (step, step), 1)
    ).astype(F32).astype(BF16)
    hots, counts = [], jnp.zeros((wins, 1), F32)
    for b in range(rows // step):
        hot = (ids[:, b * step : (b + 1) * step] == win_iota).astype(F32)
        hots.append(hot)
        counts = counts + jnp.sum(hot, axis=1, keepdims=True)
    wide = jnp.broadcast_to(counts, (wins, LANES))
    cnt_ref[...] = wide
    r_io = lax.broadcasted_iota(jnp.int32, (wins, wins), 0)
    c_io = lax.broadcasted_iota(jnp.int32, (wins, wins), 1)
    same = (r_io // WIN_DEV == c_io // WIN_DEV) & (c_io < r_io)
    carry = dot(same.astype(F32).astype(BF16), wide.astype(BF16))[:, :1]
    ranks = []
    for hot in hots:
        cum = dot(hot.astype(BF16), upper) + carry
        ranks.append(jnp.sum(hot * cum, axis=0, keepdims=True))
        carry = carry + jnp.sum(hot, axis=1, keepdims=True)
    rank = jnp.concatenate(ranks, axis=1).astype(jnp.int32)
    dest = steps.step(me, ids // WIN_DEV) * cap + rank
    col_ref[...] = jnp.transpose(jnp.broadcast_to(dest.astype(F32), (LANES, rows))).astype(jnp.int32)
    row_iota = lax.broadcasted_iota(jnp.int32, (cap, rows), 0)
    for k in range(n):
        out = outs[k]
        piece = out.shape[1]
        pick = (dest == row_iota + k * cap).astype(F32).astype(BF16)
        if k < near:
            source = normed_ref[...]
        else:
            source = normed_ref[:, pl.ds(pl.multiple_of(mp * piece, LANES), piece)]
        out[0:cap, :] = dot(pick, source).astype(BF16)
        owner = steps.to(me, k)
        tail = cnt_ref[pl.ds(pl.multiple_of(owner * WIN_DEV, WIN_DEV), WIN_DEV), :]
        out[cap : cap + META, :] = jnp.concatenate([tail] * (piece // LANES), axis=1).astype(BF16)


def places(tails, cap):
    base = jnp.zeros((META, 1), F32)
    lower = (
        lax.broadcasted_iota(jnp.int32, (META, META), 1)
        < lax.broadcasted_iota(jnp.int32, (META, META), 0)
    ).astype(F32).astype(BF16)
    row = lax.broadcasted_iota(jnp.int32, (META, cap), 1).astype(F32)
    win = lax.broadcasted_iota(jnp.int32, (META, 1), 0).astype(F32) * WLEN
    out = []
    for tail in tails:
        start = dot(lower, tail)[:, :1]
        count = tail.astype(F32)[:, :1]
        inside = (row >= start) & (row < start + count)
        value = jnp.where(inside, win + base - start + row + 1.0, 0.0)
        out.append((jnp.sum(value, axis=0, keepdims=True) - 1.0).astype(jnp.int32))
        base = base + count
    return out


def read_piece(ref, t, near, piece, cap, block):
    if near:
        return ref[0:cap, pl.ds(pl.multiple_of(block * piece, LANES), piece)]
    return ref[0:cap, :]


def place_kernel(*refs, names, parts, cap, near, mp_steps, has_prev, first, piece):
    count = len(parts)
    table = refs[-1]
    tails_refs = refs[: len(first)]
    at = len(first)
    part_refs = []
    for width in parts:
        part_refs.append(refs[at : at + width])
        at += width
    prev = refs[at] if has_prev else None
    mp = lax.axis_index("mp")
    tails = [r[cap : cap + META, 0:LANES] for r in tails_refs]
    where_all = places(tails, cap)
    picks = [where_all[i] for i in names]
    windows = table.shape[0] // WLEN
    slot = lax.broadcasted_iota(jnp.int32, (WLEN, cap), 0)

    @pl.loop(0, windows)
    def _(w):
        rows = pl.ds(pl.multiple_of(w * WLEN, WLEN), WLEN)
        hots = [(slot + w * WLEN == p).astype(F32).astype(BF16) for p in picks]
        for t in range(mp_steps.n):
            acc = prev[rows, t * piece : (t + 1) * piece].astype(F32) if has_prev else None
            block = mp_steps.frm(mp, t)
            for i in range(count):
                is_near = len(part_refs[i]) == 1
                src = part_refs[i][0] if is_near else part_refs[i][t]
                term = dot(hots[i], read_piece(src, t, is_near, piece, cap, block))
                acc = term if acc is None else acc + term
            table[rows, t * piece : (t + 1) * piece] = acc.astype(BF16)


def attend_kernel(*refs, names, parts, cap, mp_steps, first, piece, local, sub_size):
    count = len(parts)
    att, pos_ref, weight_ref = refs[-3], refs[-2], refs[-1]
    tails_refs = refs[: len(first)]
    at = len(first)
    part_refs = []
    for width in parts:
        part_refs.append(refs[at : at + width])
        at += width
    prev, wqk_ref, wv_ref, counts_ref = refs[at : at + 4]
    mp = lax.axis_index("mp")
    me = own_index(sub_size)
    tails = [r[cap : cap + META, 0:LANES] for r in tails_refs]
    where_all = places(tails, cap)
    for i, p in enumerate(where_all):
        pos_ref[i * cap : (i + 1) * cap, :] = jnp.transpose(
            jnp.broadcast_to(p.astype(F32), (LANES, cap))
        ).astype(jnp.int32)
    picks = [where_all[i] for i in names]
    for t in range(mp_steps.n):
        block = pl.ds(pl.multiple_of(mp_steps.frm(mp, t) * piece, piece), piece)
        to = slice(t * piece, (t + 1) * piece)
        weight_ref[to, 0:local] = wqk_ref[0, block, :]
        weight_ref[to, local : 2 * local] = wqk_ref[1, block, :]
        weight_ref[to, 2 * local : 3 * local] = wv_ref[block, :]
    windows = att.shape[0] // WLEN
    slot = lax.broadcasted_iota(jnp.int32, (WLEN, cap), 0)
    lane = lax.broadcasted_iota(jnp.int32, (WLEN, LANES), 1)
    low = lane < HDIM
    key = lax.broadcasted_iota(jnp.int32, (WLEN, WLEN), 1)
    factor = HDIM ** (-0.5) * 1.4426950408889634

    @pl.loop(0, windows)
    def _(w):
        rows = pl.ds(pl.multiple_of(w * WLEN, WLEN), WLEN)
        live = counts_ref[me * windows + w]

        @pl.when(live == 0)
        def _():
            att[rows, :] = jnp.zeros((WLEN, local), BF16)

        @pl.when(live > 0)
        def _():
            hots = [(slot + w * WLEN == p).astype(F32).astype(BF16) for p in picks]
            cols = []
            for t in range(mp_steps.n):
                acc = prev[rows, t * piece : (t + 1) * piece].astype(F32)
                block = mp_steps.frm(mp, t)
                for i in range(count):
                    is_near = len(part_refs[i]) == 1
                    src = part_refs[i][0] if is_near else part_refs[i][t]
                    acc = acc + dot(hots[i], read_piece(src, t, is_near, piece, cap, block))
                cols.append(acc.astype(BF16))
            members = jnp.concatenate(cols, axis=1)
            qkv = dot(members, weight_ref[...]).astype(BF16)
            zero = jnp.zeros((WLEN, LANES), BF16)
            for pair in range(local // LANES):
                q = qkv[:, pair * LANES : (pair + 1) * LANES]
                k = qkv[:, local + pair * LANES : local + (pair + 1) * LANES]
                v = qkv[:, 2 * local + pair * LANES : 2 * local + (pair + 1) * LANES]
                total, mixed = [], None
                for half in (low, ~low):
                    scores = lax.dot_general(
                        q, jnp.where(half, k, zero), (((1,), (1,)), ((), ())),
                        preferred_element_type=F32,
                    )
                    scores = jnp.where(key < live, scores, -1e30)
                    top = jnp.max(scores, axis=1, keepdims=True)
                    grown = jnp.exp2((scores - top) * factor)
                    total.append(jnp.sum(grown, axis=1, keepdims=True))
                    term = dot(grown.astype(BF16), jnp.where(half, v, zero))
                    mixed = term if mixed is None else mixed + term
                mixed = mixed / jnp.where(low, total[0], total[1])
                att[rows, pair * LANES : (pair + 1) * LANES] = mixed.astype(BF16)


def fetch_kernel(att_ref, pos_ref, *outs, names, cap):
    slots = att_ref.shape[0]
    for i, k in enumerate(names):
        pos = pos_ref[k * cap : (k + 1) * cap, :]
        lane = lax.broadcasted_iota(jnp.int32, (cap, LANES), 1)
        hot = jnp.concatenate(
            [(pos == lane + t * LANES).astype(F32).astype(BF16) for t in range(slots // LANES)],
            axis=1,
        )
        outs[i][...] = dot(hot, att_ref[...]).astype(BF16)


def final_kernel(*refs, n, cap, mp_steps, sub_size, local, block_rows):
    parts = mp_steps.n
    bucket_refs = [refs[k * parts : (k + 1) * parts] for k in range(n)]
    at = n * parts
    col_ref, vox_ref, gain_ref, wout_ref, wup_ref, wdown_ref = refs[at : at + 6]
    at += 6
    extra = refs[at : at + 3 * sub_size * (parts - 1)]
    out_ref, proj_ref = refs[-2], refs[-1]
    mp = lax.axis_index("mp")
    sub = lax.axis_index("sub")
    width = vox_ref.shape[1]
    out_width = out_ref.shape[1]
    mine = pl.ds(pl.multiple_of(mp * out_width, LANES), out_width)
    proj_ref[0:local, :] = wout_ref[...]
    ups, downs = [wup_ref], [None]
    part_rows = local // sub_size
    for t in range(1, parts):
        for j in range(sub_size):
            up, down, proj = extra[3 * ((t - 1) * sub_size + j) : 3 * ((t - 1) * sub_size + j) + 3]
            ups.append(up)
            downs.append(down)
            at_row = t * local + (sub + j) % sub_size * part_rows
            proj_ref[pl.ds(pl.multiple_of(at_row, part_rows), part_rows), :] = proj[...]
    rows_total = vox_ref.shape[0]
    lane = lax.broadcasted_iota(jnp.int32, (block_rows, LANES), 1)

    @pl.loop(0, rows_total // block_rows)
    def _(b):
        rows = pl.ds(pl.multiple_of(b * block_rows, block_rows), block_rows)
        dest = col_ref[rows, :]
        heads = [None] * parts
        for k in range(n):
            base = k * cap
            tiles = []
            for t in range(-(-cap // LANES)):
                tiles.append((dest == lane + (base + t * LANES)).astype(F32).astype(BF16))
            hot = tiles[0] if len(tiles) == 1 else jnp.concatenate(tiles, axis=1)
            hot = hot[:, 0:cap]
            for t in range(parts):
                term = dot(hot, bucket_refs[k][t][...])
                heads[t] = term if heads[t] is None else heads[t] + term
        every = jnp.concatenate([h.astype(BF16) for h in heads], axis=1)
        after = vox_ref[rows, :].astype(F32) + dot(every, proj_ref[...])
        normed = layer_norm(after, gain_ref[...]).astype(BF16)
        total = None
        for up, down in zip(ups, downs):
            u = dot(normed, up[...])
            inner = 0.7978845608028654 * (u + 0.044715 * u * u * u)
            hidden = (0.5 * u * (1.0 + jnp.tanh(inner))).astype(BF16)
            term = dot(hidden, wdown_ref[:, mine] if down is None else down[...])
            total = term if total is None else total + term
        keep = jnp.zeros((block_rows, out_width), F32)
        for j in range(width // out_width):
            keep = jnp.where(mp == j, after[:, j * out_width : (j + 1) * out_width], keep)
        out_ref[rows, :] = (keep + total).astype(BF16)


def shards(
    voxels, window_ids, voxel_slots, window_counts, norm_gain, w_query_key, w_value, w_out,
    ffn_gain, w_up, w_down, *, n, mp_size, sub_size,
):
    rows, width = voxels.shape
    cap = 2 * rows // n
    steps, mp_steps = Steps(n), Steps(mp_size)
    near = sub_size if steps.xor else 1
    piece = width // mp_size
    local = w_value.shape[1]
    mp = lax.axis_index("mp")
    sub = lax.axis_index("sub")
    wins = n * WIN_DEV

    def over_mp(x, t):
        return lax.ppermute(x, "mp", mp_steps.perm(t))

    hidden = w_up.shape[1]
    part = hidden // sub_size
    out_part = w_out.shape[0] // sub_size
    extra = []
    for t in range(1, mp_size):
        to = mp_steps.to(mp, t)
        up = over_mp(lax.dynamic_slice_in_dim(w_up, sub * part, part, 1), t)
        down = over_mp(lax.dynamic_slice(w_down, (sub * part, to * piece), (part, piece)), t)
        proj = over_mp(lax.dynamic_slice_in_dim(w_out, sub * out_part, out_part, 0), t)
        extra += [up, down, proj]
        for j in range(1, sub_size):
            share = [((i + j) % sub_size, i) for i in range(sub_size)]
            extra += [lax.ppermute(x, "sub", share) for x in (up, down, proj)]

    bucket = cap + META
    packed = pl.pallas_call(
        functools.partial(
            pack_kernel, steps=steps, sub_size=sub_size, near=near, cap=cap, wins=wins
        ),
        out_shape=[jax.ShapeDtypeStruct((rows, LANES), jnp.int32)]
        + [jax.ShapeDtypeStruct((bucket, width if k < near else piece), BF16) for k in range(n)],
        in_specs=[VM] * 3,
        out_specs=[VM] * (n + 1),
        scratch_shapes=[pltpu.VMEM((rows, width), BF16), pltpu.VMEM((wins, LANES), F32)],
        compiler_params=PARAMS,
        name="pack",
    )(window_ids.reshape(1, rows), voxels, norm_gain.reshape(1, width))
    dest_col, packed = packed[0], packed[1:]

    far = list(range(near, n))
    if n == 8 and near == 2:
        far = [4, 2, 5, 3, 6, 7]
    arrived = {k: [lax.ppermute(packed[k], OWN, steps.perm(k))] for k in range(1, near)}
    arrived[0] = [packed[0]]
    for i, k in enumerate(far):
        sent = packed[k]
        if i >= 2:
            sent, _ = lax.optimization_barrier((sent, arrived[far[i - 2]][0]))
        got = lax.ppermute(sent, OWN, steps.perm(k))
        arrived[k] = [got] + [over_mp(got, t) for t in range(1, mp_size)]

    order = list(range(near)) + far
    late = order[-2:]
    early = order[:-2]

    def gather_args(group, upto):
        first = order[: upto]
        tails = [arrived[k][0] for k in first]
        parts = [len(arrived[k]) for k in group]
        names = [first.index(k) for k in group]
        flat = [x for k in group for x in arrived[k]]
        return first, tails, parts, names, flat

    slots = WIN_DEV * WLEN
    first, tails, parts, names, flat = gather_args(early, len(early))
    table = pl.pallas_call(
        functools.partial(
            place_kernel, names=names, parts=parts, cap=cap, near=near, mp_steps=mp_steps,
            has_prev=False, first=first, piece=piece,
        ),
        out_shape=jax.ShapeDtypeStruct((slots, width), BF16),
        in_specs=[VM] * (len(tails) + len(flat)),
        out_specs=VM,
        compiler_params=PARAMS,
        name="place",
    )(*tails, *flat)
    first, tails, parts, names, flat = gather_args(late, len(order))
    att, pos = pl.pallas_call(
        functools.partial(
            attend_kernel, names=names, parts=parts, cap=cap, mp_steps=mp_steps, first=first,
            piece=piece, local=local, sub_size=sub_size,
        ),
        out_shape=[
            jax.ShapeDtypeStruct((slots, local), BF16),
            jax.ShapeDtypeStruct((n * cap, LANES), jnp.int32),
        ],
        in_specs=[VM] * (len(tails) + len(flat) + 3)
        + [pl.BlockSpec(memory_space=pltpu.SMEM)],
        out_specs=[VM, VM],
        scratch_shapes=[pltpu.VMEM((width, 3 * local), BF16)],
        compiler_params=PARAMS,
        name="attend",
    )(*tails, *flat, table, w_query_key, w_value, window_counts)

    answers = {}
    for group in (far[:2], [0, 1][:near] + far[2:]):
        got = pl.pallas_call(
            functools.partial(fetch_kernel, names=[order.index(k) for k in group], cap=cap),
            out_shape=[jax.ShapeDtypeStruct((cap, local), BF16) for _ in group],
            in_specs=[VM, VM],
            out_specs=[VM] * len(group),
            compiler_params=PARAMS,
            name="fetch",
        )(att, pos)
        answers.update(zip(group, got))
    returned = {}
    for k in range(near):
        home = answers[k] if k == 0 else lax.ppermute(answers[k], OWN, steps.perm(k, True))
        returned[k] = [home] + [over_mp(home, t) for t in range(1, mp_size)]
    for i, k in enumerate(far):
        sent = answers[k]
        if i >= 2:
            sent, _ = lax.optimization_barrier((sent, returned[far[i - 2]][0]))
        home = lax.ppermute(sent, OWN, steps.perm(k, True))
        returned[k] = [home] + [over_mp(home, t) for t in range(1, mp_size)]

    flat = [x for k in range(n) for x in returned[k]]
    return pl.pallas_call(
        functools.partial(
            final_kernel, n=n, cap=cap, mp_steps=mp_steps, sub_size=sub_size, local=local,
            block_rows=256,
        ),
        out_shape=jax.ShapeDtypeStruct((rows, piece), BF16),
        in_specs=[VM] * (len(flat) + 6 + len(extra)),
        out_specs=VM,
        scratch_shapes=[pltpu.VMEM((mp_size * local, width), BF16)],
        compiler_params=PARAMS,
        name="final",
    )(*flat, dest_col, voxels, ffn_gain.reshape(1, width), w_out, w_up, w_down, *extra)


def solution(mesh):
    sizes = mesh.shape
    body = functools.partial(
        shards, n=sizes["space"] * sizes["sub"], mp_size=sizes["mp"], sub_size=sizes["sub"]
    )
    return jax.shard_map(
        body,
        mesh=mesh,
        in_specs=(
            P(("groups", "space", "sub"), None),
            P(("groups", "space", "sub")),
            P(("groups", "space", "sub")),
            P("groups"),
            P(),
            P(None, None, "mp"),
            P(None, "mp"),
            P("mp", None),
            P(),
            P(None, "mp"),
            P("mp", None),
        ),
        out_specs=P(("groups", "space", "sub"), "mp"),
        check_vma=False,
    )
```

```python
import functools

import jax
import jax.numpy as jnp
from jax import lax
from jax.experimental import pallas as pl
from jax.experimental.pallas import tpu as pltpu
from jax.sharding import PartitionSpec as P


HDIM = 64
WLEN = 256
WIN_DEV = 16
META = 16
LANES = 128
OWN = ("space", "sub")


F32 = jnp.float32
BF16 = jnp.bfloat16
VM = pl.BlockSpec(memory_space=pltpu.VMEM)
PARAMS = pltpu.CompilerParams(vmem_limit_bytes=20 * 1024 * 1024)


class Steps:
    def __init__(self, n):
        self.n = n
        self.xor = n & (n - 1) == 0

    def to(self, i, k):
        return i ^ k if self.xor else (i + k) % self.n

    def frm(self, i, k):
        return i ^ k if self.xor else (i + self.n - k) % self.n

    def step(self, i, owner):
        return owner ^ i if self.xor else (owner + self.n - i) % self.n

    def perm(self, k, back=False):
        go = self.frm if back else self.to
        return [(i, go(i, k)) for i in range(self.n)]


def layer_norm(values_in, gain):
    row_mean = jnp.mean(values_in, axis=-1, keepdims=True)
    centred = values_in - row_mean
    variance = jnp.mean(centred * centred, axis=-1, keepdims=True)
    return centred * lax.rsqrt(variance + 1e-05) * gain


def dot(a, b):
    return jnp.dot(a, b, preferred_element_type=F32)


def own_index(sub_size):
    return lax.axis_index("space") * sub_size + lax.axis_index("sub")


def pack_kernel(ids_ref, vox_ref, gain_ref, *refs, steps, sub_size, near, cap, wins):
    n = steps.n
    col_ref, outs, normed_ref, cnt_ref = refs[0], refs[1 : 1 + n], refs[1 + n], refs[2 + n]
    rows, _ = vox_ref.shape
    me = own_index(sub_size)
    mp = lax.axis_index("mp")
    normed_ref[...] = layer_norm(vox_ref[...].astype(F32), gain_ref[...]).astype(BF16)
    ids = ids_ref[...]
    step = 256
    win_iota = lax.broadcasted_iota(jnp.int32, (wins, step), 0)
    upper = (
        lax.broadcasted_iota(jnp.int32, (step, step), 0)
        < lax.broadcasted_iota(jnp.int32, (step, step), 1)
    ).astype(F32).astype(BF16)
    hots, counts = [], jnp.zeros((wins, 1), F32)
    for b in range(rows // step):
        hot = (ids[:, b * step : (b + 1) * step] == win_iota).astype(F32)
        hots.append(hot)
        counts = counts + jnp.sum(hot, axis=1, keepdims=True)
    wide = jnp.broadcast_to(counts, (wins, LANES))
    cnt_ref[...] = wide
    r_io = lax.broadcasted_iota(jnp.int32, (wins, wins), 0)
    c_io = lax.broadcasted_iota(jnp.int32, (wins, wins), 1)
    same = (r_io // WIN_DEV == c_io // WIN_DEV) & (c_io < r_io)
    carry = dot(same.astype(F32).astype(BF16), wide.astype(BF16))[:, :1]
    ranks = []
    for hot in hots:
        cum = dot(hot.astype(BF16), upper) + carry
        ranks.append(jnp.sum(hot * cum, axis=0, keepdims=True))
        carry = carry + jnp.sum(hot, axis=1, keepdims=True)
    rank = jnp.concatenate(ranks, axis=1).astype(jnp.int32)
    dest = steps.step(me, ids // WIN_DEV) * cap + rank
    col_ref[...] = jnp.transpose(jnp.broadcast_to(dest.astype(F32), (LANES, rows))).astype(jnp.int32)
    row_iota = lax.broadcasted_iota(jnp.int32, (cap, rows), 0)
    for k in range(n):
        out = outs[k]
        piece = out.shape[1]
        pick = (dest == row_iota + k * cap).astype(F32).astype(BF16)
        if k < near:
            source = normed_ref[...]
        else:
            source = normed_ref[:, pl.ds(pl.multiple_of(mp * piece, LANES), piece)]
        out[0:cap, :] = dot(pick, source).astype(BF16)
        owner = steps.to(me, k)
        tail = cnt_ref[pl.ds(pl.multiple_of(owner * WIN_DEV, WIN_DEV), WIN_DEV), :]
        out[cap : cap + META, :] = jnp.concatenate([tail] * (piece // LANES), axis=1).astype(BF16)


def places(tails, cap):
    base = jnp.zeros((META, 1), F32)
    lower = (
        lax.broadcasted_iota(jnp.int32, (META, META), 1)
        < lax.broadcasted_iota(jnp.int32, (META, META), 0)
    ).astype(F32).astype(BF16)
    row = lax.broadcasted_iota(jnp.int32, (META, cap), 1).astype(F32)
    win = lax.broadcasted_iota(jnp.int32, (META, 1), 0).astype(F32) * WLEN
    out = []
    for tail in tails:
        start = dot(lower, tail)[:, :1]
        count = tail.astype(F32)[:, :1]
        inside = (row >= start) & (row < start + count)
        value = jnp.where(inside, win + base - start + row + 1.0, 0.0)
        out.append((jnp.sum(value, axis=0, keepdims=True) - 1.0).astype(jnp.int32))
        base = base + count
    return out


def read_piece(refs, t, piece, cap, block):
    if len(refs) == 1:
        return refs[0][0:cap, pl.ds(pl.multiple_of(block * piece, LANES), piece)]
    return refs[t][0:cap, :]


def window_bits(tail):
    power = jnp.left_shift(1, lax.broadcasted_iota(jnp.int32, (META, LANES), 0)).astype(F32)
    lane = lax.broadcasted_iota(jnp.int32, (META, LANES), 1)
    return jnp.sum(jnp.where((tail.astype(F32) > 0) & (lane == 0), power, 0.0)).astype(jnp.int32)


def split_refs(refs, at, parts):
    out = []
    for width in parts:
        out.append(refs[at : at + width])
        at += width
    return out, at


def add_rows(dest, hot, part, mp, mp_steps, piece, cap):
    for t in range(mp_steps.n):
        cols = slice(t * piece, (t + 1) * piece)
        term = dot(hot, read_piece(part, t, piece, cap, mp_steps.frm(mp, t)))
        dest[:, cols] = dest[:, cols] + term.astype(BF16)


def place_kernel(*refs, names, parts, cap, mp_steps, tails_count, piece):
    table = refs[-1]
    part_refs, _ = split_refs(refs, tails_count, parts)
    mp = lax.axis_index("mp")
    tails = [r[cap : cap + META, 0:LANES] for r in refs[:tails_count]]
    where_all = places(tails, cap)
    bits = [window_bits(tails[i]) for i in names]
    slot = lax.broadcasted_iota(jnp.int32, (WLEN, cap), 0)

    @pl.loop(0, table.shape[0] // WLEN)
    def _(w):
        rows = table.at[pl.ds(pl.multiple_of(w * WLEN, WLEN), WLEN), :]
        rows[...] = jnp.zeros(rows.shape, BF16)
        for i, name in enumerate(names):

            @pl.when((bits[i] >> w) & 1 == 1)
            def _():
                hot = (slot + w * WLEN == where_all[name]).astype(F32).astype(BF16)
                add_rows(rows, hot, part_refs[i], mp, mp_steps, piece, cap)


def attend_kernel(*refs, names, parts, cap, mp_steps, tails_count, piece, local, sub_size):
    att, pos_ref, weight_ref, member_ref = refs[-4:]
    part_refs, at = split_refs(refs, tails_count, parts)
    table_ref, wqk_ref, wv_ref, counts_ref = refs[at : at + 4]
    mp = lax.axis_index("mp")
    me = own_index(sub_size)
    tails = [r[cap : cap + META, 0:LANES] for r in refs[:tails_count]]
    where_all = places(tails, cap)
    bits = [window_bits(tails[i]) for i in names]
    for i, p in enumerate(where_all):
        pos_ref[i * cap : (i + 1) * cap, :] = jnp.transpose(
            jnp.broadcast_to(p.astype(F32), (LANES, cap))
        ).astype(jnp.int32)
    for t in range(mp_steps.n):
        block = pl.ds(pl.multiple_of(mp_steps.frm(mp, t) * piece, piece), piece)
        to = slice(t * piece, (t + 1) * piece)
        weight_ref[to, 0:local] = wqk_ref[0, block, :]
        weight_ref[to, local : 2 * local] = wqk_ref[1, block, :]
        weight_ref[to, 2 * local : 3 * local] = wv_ref[block, :]
    windows = att.shape[0] // WLEN
    slot = lax.broadcasted_iota(jnp.int32, (WLEN, cap), 0)
    low = lax.broadcasted_iota(jnp.int32, (WLEN, LANES), 1) < HDIM
    key = lax.broadcasted_iota(jnp.int32, (WLEN, WLEN), 1)
    factor = HDIM ** (-0.5) * 1.4426950408889634

    @pl.loop(0, windows)
    def _(w):
        rows = pl.ds(pl.multiple_of(w * WLEN, WLEN), WLEN)
        live = counts_ref[me * windows + w]

        @pl.when(live == 0)
        def _():
            att[rows, :] = jnp.zeros((WLEN, local), BF16)

        @pl.when(live > 0)
        def _():
            member_ref[...] = table_ref[rows, :]
            for i, name in enumerate(names):

                @pl.when((bits[i] >> w) & 1 == 1)
                def _():
                    hot = (slot + w * WLEN == where_all[name]).astype(F32).astype(BF16)
                    add_rows(member_ref, hot, part_refs[i], mp, mp_steps, piece, cap)

            qkv = dot(member_ref[...], weight_ref[...]).astype(BF16)
            zero = jnp.zeros((WLEN, LANES), BF16)
            for pair in range(local // LANES):
                q = qkv[:, pair * LANES : (pair + 1) * LANES]
                k = qkv[:, local + pair * LANES : local + (pair + 1) * LANES]
                v = qkv[:, 2 * local + pair * LANES : 2 * local + (pair + 1) * LANES]
                total, mixed = [], None
                for half in (low, ~low):
                    scores = lax.dot_general(
                        q, jnp.where(half, k, zero), (((1,), (1,)), ((), ())),
                        preferred_element_type=F32,
                    )
                    scores = jnp.where(key < live, scores, -1e30)
                    top = jnp.max(scores, axis=1, keepdims=True)
                    grown = jnp.exp2((scores - top) * factor)
                    total.append(jnp.sum(grown, axis=1, keepdims=True))
                    term = dot(grown.astype(BF16), jnp.where(half, v, zero))
                    mixed = term if mixed is None else mixed + term
                mixed = mixed / jnp.where(low, total[0], total[1])
                att[rows, pair * LANES : (pair + 1) * LANES] = mixed.astype(BF16)


def fetch_kernel(att_ref, pos_ref, *outs, names, cap):
    slots = att_ref.shape[0]
    for i, k in enumerate(names):
        pos = pos_ref[k * cap : (k + 1) * cap, :]
        lane = lax.broadcasted_iota(jnp.int32, (cap, LANES), 1)
        hot = jnp.concatenate(
            [(pos == lane + t * LANES).astype(F32).astype(BF16) for t in range(slots // LANES)],
            axis=1,
        )
        outs[i][...] = dot(hot, att_ref[...]).astype(BF16)


def spots(dest, lane, base, cap):
    tiles = []
    for t in range(-(-cap // LANES)):
        tiles.append((dest == lane + (base + t * LANES)).astype(F32).astype(BF16))
    hot = tiles[0] if len(tiles) == 1 else jnp.concatenate(tiles, axis=1)
    return hot[:, 0:cap]


def unpack_kernel(*refs, names, cap, parts, local, block_rows):
    col_ref, out_ref = refs[-2], refs[-1]
    lane = lax.broadcasted_iota(jnp.int32, (block_rows, LANES), 1)

    @pl.loop(0, out_ref.shape[0] // block_rows)
    def _(b):
        rows = pl.ds(pl.multiple_of(b * block_rows, block_rows), block_rows)
        dest = col_ref[rows, :]
        heads = [None] * parts
        for i, k in enumerate(names):
            hot = spots(dest, lane, k * cap, cap)
            for t in range(parts):
                term = dot(hot, refs[i * parts + t][...])
                heads[t] = term if heads[t] is None else heads[t] + term
        for t in range(parts):
            out_ref[rows, t * local : (t + 1) * local] = heads[t].astype(BF16)


def final_kernel(*refs, names, cap, mp_steps, sub_size, local, block_rows):
    parts = mp_steps.n
    at = len(names) * parts
    early_ref, col_ref, vox_ref, gain_ref, wout_ref, wup_ref, wdown_ref = refs[at : at + 7]
    at += 7
    extra = refs[at : at + 3 * sub_size * (parts - 1)]
    out_ref, proj_ref = refs[-2], refs[-1]
    mp = lax.axis_index("mp")
    sub = lax.axis_index("sub")
    width = vox_ref.shape[1]
    out_width = out_ref.shape[1]
    mine = pl.ds(pl.multiple_of(mp * out_width, LANES), out_width)
    proj_ref[0:local, :] = wout_ref[...]
    ups, downs = [wup_ref], [None]
    part_rows = local // sub_size
    for t in range(1, parts):
        for j in range(sub_size):
            up, down, proj = extra[3 * ((t - 1) * sub_size + j) : 3 * ((t - 1) * sub_size + j) + 3]
            ups.append(up)
            downs.append(down)
            at_row = t * local + (sub + j) % sub_size * part_rows
            proj_ref[pl.ds(pl.multiple_of(at_row, part_rows), part_rows), :] = proj[...]
    lane = lax.broadcasted_iota(jnp.int32, (block_rows, LANES), 1)

    @pl.loop(0, vox_ref.shape[0] // block_rows)
    def _(b):
        rows = pl.ds(pl.multiple_of(b * block_rows, block_rows), block_rows)
        dest = col_ref[rows, :]
        heads = [early_ref[rows, t * local : (t + 1) * local].astype(F32) for t in range(parts)]
        for i, k in enumerate(names):
            hot = spots(dest, lane, k * cap, cap)
            for t in range(parts):
                heads[t] = heads[t] + dot(hot, refs[i * parts + t][...])
        every = jnp.concatenate([h.astype(BF16) for h in heads], axis=1)
        after = vox_ref[rows, :].astype(F32) + dot(every, proj_ref[...])
        normed = layer_norm(after, gain_ref[...]).astype(BF16)
        total = None
        for up, down in zip(ups, downs):
            u = dot(normed, up[...])
            inner = u * (0.7978845608028654 + (0.7978845608028654 * 0.044715) * (u * u))
            half = 0.5 * u
            hidden = (half + half * jnp.tanh(inner)).astype(BF16)
            term = dot(hidden, wdown_ref[:, mine] if down is None else down[...])
            total = term if total is None else total + term
        keep = after[:, 0:out_width]
        for j in range(1, width // out_width):
            keep = jnp.where(mp == j, after[:, j * out_width : (j + 1) * out_width], keep)
        out_ref[rows, :] = (keep + total).astype(BF16)


def far_order(n, near):
    if n == 8 and near == 2:
        return [4, 2, 5, 3, 6, 7]
    return list(range(near, n))


def near_count(n, sub_size):
    return sub_size if Steps(n).xor else 1


def shards(
    voxels, window_ids, voxel_slots, window_counts, norm_gain, w_query_key, w_value, w_out,
    ffn_gain, w_up, w_down, *, n, mp_size, sub_size,
):
    rows, width = voxels.shape
    cap = 2 * rows // n
    steps, mp_steps = Steps(n), Steps(mp_size)
    near = near_count(n, sub_size)
    far = far_order(n, near)
    order = list(range(near)) + far
    early, late = order[:-2], order[-2:]
    piece = width // mp_size
    local = w_value.shape[1]
    mp = lax.axis_index("mp")
    sub = lax.axis_index("sub")

    def over_mp(x, t):
        return lax.ppermute(x, "mp", mp_steps.perm(t))

    bucket = cap + META
    packed = pl.pallas_call(
        functools.partial(
            pack_kernel, steps=steps, sub_size=sub_size, near=near, cap=cap, wins=n * WIN_DEV
        ),
        out_shape=[jax.ShapeDtypeStruct((rows, LANES), jnp.int32)]
        + [jax.ShapeDtypeStruct((bucket, width if k < near else piece), BF16) for k in range(n)],
        in_specs=[VM] * 3,
        out_specs=[VM] * (n + 1),
        scratch_shapes=[pltpu.VMEM((rows, width), BF16), pltpu.VMEM((n * WIN_DEV, LANES), F32)],
        compiler_params=PARAMS,
        name="pack",
    )(window_ids.reshape(1, rows), voxels, norm_gain.reshape(1, width))
    dest_col, packed = packed[0], packed[1:]

    arrived = {0: [packed[0]]}
    for k in range(1, near):
        arrived[k] = [lax.ppermute(packed[k], OWN, steps.perm(k))]
    for i, k in enumerate(far):
        sent = packed[k]
        if i >= 2:
            sent, _ = lax.optimization_barrier((sent, arrived[far[i - 2]][0]))
        got = lax.ppermute(sent, OWN, steps.perm(k))
        arrived[k] = [got] + [over_mp(got, t) for t in range(1, mp_size)]

    part = w_up.shape[1] // sub_size
    out_part = w_out.shape[0] // sub_size
    extra = []
    for t in range(1, mp_size):
        to = mp_steps.to(mp, t)
        up = over_mp(lax.dynamic_slice_in_dim(w_up, sub * part, part, 1), t)
        down = over_mp(lax.dynamic_slice(w_down, (sub * part, to * piece), (part, piece)), t)
        proj = over_mp(lax.dynamic_slice_in_dim(w_out, sub * out_part, out_part, 0), t)
        extra += [up, down, proj]
        for j in range(1, sub_size):
            share = [((i + j) % sub_size, i) for i in range(sub_size)]
            extra += [lax.ppermute(x, "sub", share) for x in (up, down, proj)]

    slots = WIN_DEV * WLEN
    flat = [x for k in early for x in arrived[k]]
    table = pl.pallas_call(
        functools.partial(
            place_kernel, names=list(range(len(early))), parts=[len(arrived[k]) for k in early],
            cap=cap, mp_steps=mp_steps, tails_count=len(early), piece=piece,
        ),
        out_shape=jax.ShapeDtypeStruct((slots, width), BF16),
        in_specs=[VM] * (len(early) + len(flat)),
        out_specs=VM,
        compiler_params=PARAMS,
        name="place",
    )(*[arrived[k][0] for k in early], *flat)
    flat = [x for k in late for x in arrived[k]]
    att, pos = pl.pallas_call(
        functools.partial(
            attend_kernel, names=[order.index(k) for k in late],
            parts=[len(arrived[k]) for k in late], cap=cap, mp_steps=mp_steps, tails_count=n,
            piece=piece, local=local, sub_size=sub_size,
        ),
        out_shape=[
            jax.ShapeDtypeStruct((slots, local), BF16),
            jax.ShapeDtypeStruct((n * cap, LANES), jnp.int32),
        ],
        in_specs=[VM] * (n + len(flat) + 3) + [pl.BlockSpec(memory_space=pltpu.SMEM)],
        out_specs=[VM, VM],
        scratch_shapes=[pltpu.VMEM((width, 3 * local), BF16), pltpu.VMEM((WLEN, width), BF16)],
        compiler_params=PARAMS,
        name="attend",
    )(*[arrived[k][0] for k in order], *flat, table, w_query_key, w_value, window_counts)

    answers = {}
    for group in (far[:2], list(range(near)) + far[2:]):
        got = pl.pallas_call(
            functools.partial(fetch_kernel, names=[order.index(k) for k in group], cap=cap),
            out_shape=[jax.ShapeDtypeStruct((cap, local), BF16) for _ in group],
            in_specs=[VM, VM],
            out_specs=[VM] * len(group),
            compiler_params=PARAMS,
            name="fetch",
        )(att, pos)
        answers.update(zip(group, got))
    returned = {}
    for i, k in enumerate(order):
        home = answers[k]
        if i >= near + 2:
            home, _ = lax.optimization_barrier((home, returned[order[i - 2]][0]))
        if k > 0:
            home = lax.ppermute(home, OWN, steps.perm(k, True))
        returned[k] = [home] + [over_mp(home, t) for t in range(1, mp_size)]

    block_rows = rows // 2
    flat = [x for k in early for x in returned[k]]
    heads = pl.pallas_call(
        functools.partial(
            unpack_kernel, names=early, cap=cap, parts=mp_size, local=local,
            block_rows=block_rows,
        ),
        out_shape=jax.ShapeDtypeStruct((rows, mp_size * local), BF16),
        in_specs=[VM] * (len(flat) + 1),
        out_specs=VM,
        compiler_params=PARAMS,
        name="unpack",
    )(*flat, dest_col)
    flat = [x for k in late for x in returned[k]]
    return pl.pallas_call(
        functools.partial(
            final_kernel, names=late, cap=cap, mp_steps=mp_steps, sub_size=sub_size, local=local,
            block_rows=block_rows,
        ),
        out_shape=jax.ShapeDtypeStruct((rows, piece), BF16),
        in_specs=[VM] * (len(flat) + 7 + len(extra)),
        out_specs=VM,
        scratch_shapes=[pltpu.VMEM((mp_size * local, width), BF16)],
        compiler_params=PARAMS,
        name="final",
    )(*flat, heads, dest_col, voxels, ffn_gain.reshape(1, width), w_out, w_up, w_down, *extra)


def solution(mesh):
    sizes = mesh.shape
    n, sub_size = sizes["space"] * sizes["sub"], sizes["sub"]

    def body(*args):
        return shards(*args, n=n, mp_size=sizes["mp"], sub_size=sub_size)

    return jax.shard_map(
        body,
        mesh=mesh,
        in_specs=(
            P(("groups", "space", "sub"), None),
            P(("groups", "space", "sub")),
            P(("groups", "space", "sub")),
            P("groups"),
            P(),
            P(None, None, "mp"),
            P(None, "mp"),
            P("mp", None),
            P(),
            P(None, "mp"),
            P("mp", None),
        ),
        out_specs=P(("groups", "space", "sub"), "mp"),
        check_vma=False,
    )
```

```python
import functools

import jax
import jax.numpy as jnp
from jax import lax
from jax.experimental import pallas as pl
from jax.experimental.pallas import tpu as pltpu
from jax.sharding import PartitionSpec as P


HDIM = 64
WLEN = 256
WIN_DEV = 16
META = 16
LANES = 128
OWN = ("space", "sub")


F32 = jnp.float32
BF16 = jnp.bfloat16
VM = pl.BlockSpec(memory_space=pltpu.VMEM)
HB = pl.BlockSpec(memory_space=pltpu.MemorySpace.HBM)
SM = pl.BlockSpec(memory_space=pltpu.SMEM)
PARAMS = pltpu.CompilerParams(vmem_limit_bytes=20 * 1024 * 1024)


class Steps:
    def __init__(self, n):
        self.n = n
        self.xor = n & (n - 1) == 0

    def to(self, i, k):
        return i ^ k if self.xor else (i + k) % self.n

    def frm(self, i, k):
        return i ^ k if self.xor else (i + self.n - k) % self.n

    def step(self, i, owner):
        return owner ^ i if self.xor else (owner + self.n - i) % self.n

    def perm(self, k, back=False):
        go = self.frm if back else self.to
        return [(i, go(i, k)) for i in range(self.n)]


def layer_norm(values_in, gain):
    row_mean = jnp.mean(values_in, axis=-1, keepdims=True)
    centred = values_in - row_mean
    variance = jnp.mean(centred * centred, axis=-1, keepdims=True)
    return centred * lax.rsqrt(variance + 1e-05) * gain


def dot(a, b):
    return jnp.dot(a, b, preferred_element_type=F32)


def own_index(sub_size):
    return lax.axis_index("space") * sub_size + lax.axis_index("sub")


def pack_kernel(ids_ref, vox_hbm, gain_hbm, *refs, steps, sub_size, near, cap, wins):
    n = steps.n
    col_ref, outs = refs[0], refs[1 : 1 + n]
    normed_ref, cnt_ref, vox_ref, gain_ref, sem, sem_gain = refs[1 + n :]
    rows, _ = vox_ref.shape
    me = own_index(sub_size)
    mp = lax.axis_index("mp")
    load = pltpu.make_async_copy(vox_hbm, vox_ref, sem)
    load.start()
    load_gain = pltpu.make_async_copy(gain_hbm, gain_ref, sem_gain)
    load_gain.start()
    ids = ids_ref[...]
    step = 256
    win_iota = lax.broadcasted_iota(jnp.int32, (wins, step), 0)
    upper = (
        lax.broadcasted_iota(jnp.int32, (step, step), 0)
        < lax.broadcasted_iota(jnp.int32, (step, step), 1)
    ).astype(F32).astype(BF16)
    hots, counts = [], jnp.zeros((wins, 1), F32)
    for b in range(rows // step):
        hot = (ids[:, b * step : (b + 1) * step] == win_iota).astype(F32)
        hots.append(hot)
        counts = counts + jnp.sum(hot, axis=1, keepdims=True)
    wide = jnp.broadcast_to(counts, (wins, LANES))
    cnt_ref[...] = wide
    r_io = lax.broadcasted_iota(jnp.int32, (wins, wins), 0)
    c_io = lax.broadcasted_iota(jnp.int32, (wins, wins), 1)
    same = (r_io // WIN_DEV == c_io // WIN_DEV) & (c_io < r_io)
    carry = dot(same.astype(F32).astype(BF16), wide.astype(BF16))[:, :1]
    ranks = []
    for hot in hots:
        cum = dot(hot.astype(BF16), upper) + carry
        ranks.append(jnp.sum(hot * cum, axis=0, keepdims=True))
        carry = carry + jnp.sum(hot, axis=1, keepdims=True)
    rank = jnp.concatenate(ranks, axis=1).astype(jnp.int32)
    dest = steps.step(me, ids // WIN_DEV) * cap + rank
    col_ref[...] = jnp.transpose(jnp.broadcast_to(dest.astype(F32), (LANES, rows))).astype(jnp.int32)
    row_iota = lax.broadcasted_iota(jnp.int32, (cap, rows), 0)
    load_gain.wait()
    load.wait()
    normed_ref[...] = layer_norm(vox_ref[...].astype(F32), gain_ref[...]).astype(BF16)
    for k in range(n):
        out = outs[k]
        piece = out.shape[1]
        pick = (dest == row_iota + k * cap).astype(F32).astype(BF16)
        if k < near:
            source = normed_ref[...]
        else:
            source = normed_ref[:, pl.ds(pl.multiple_of(mp * piece, LANES), piece)]
        out[0:cap, :] = dot(pick, source).astype(BF16)
        owner = steps.to(me, k)
        tail = cnt_ref[pl.ds(pl.multiple_of(owner * WIN_DEV, WIN_DEV), WIN_DEV), :]
        out[cap : cap + META, :] = jnp.concatenate([tail] * (piece // LANES), axis=1).astype(BF16)


def places(tails, cap):
    base = jnp.zeros((META, 1), F32)
    lower = (
        lax.broadcasted_iota(jnp.int32, (META, META), 1)
        < lax.broadcasted_iota(jnp.int32, (META, META), 0)
    ).astype(F32).astype(BF16)
    row = lax.broadcasted_iota(jnp.int32, (META, cap), 1).astype(F32)
    win = lax.broadcasted_iota(jnp.int32, (META, 1), 0).astype(F32) * WLEN
    out = []
    for tail in tails:
        start = dot(lower, tail)[:, :1]
        count = tail.astype(F32)[:, :1]
        inside = (row >= start) & (row < start + count)
        value = jnp.where(inside, win + base - start + row + 1.0, 0.0)
        out.append((jnp.sum(value, axis=0, keepdims=True) - 1.0).astype(jnp.int32))
        base = base + count
    return out


def read_piece(refs, t, piece, cap, block):
    if len(refs) == 1:
        return refs[0][0:cap, pl.ds(pl.multiple_of(block * piece, LANES), piece)]
    return refs[t][0:cap, :]


def window_bits(tail):
    power = jnp.left_shift(1, lax.broadcasted_iota(jnp.int32, (META, LANES), 0)).astype(F32)
    lane = lax.broadcasted_iota(jnp.int32, (META, LANES), 1)
    return jnp.sum(jnp.where((tail.astype(F32) > 0) & (lane == 0), power, 0.0)).astype(jnp.int32)


def split_refs(refs, at, parts):
    out = []
    for width in parts:
        out.append(refs[at : at + width])
        at += width
    return out, at


def add_rows(dest, hot, part, mp, mp_steps, piece, cap):
    for t in range(mp_steps.n):
        cols = slice(t * piece, (t + 1) * piece)
        term = dot(hot, read_piece(part, t, piece, cap, mp_steps.frm(mp, t)))
        dest[:, cols] = dest[:, cols] + term.astype(BF16)


def place_kernel(*refs, names, parts, cap, mp_steps, tails_count, piece, has_prev, with_pos):
    table, pos_ref = refs[-2:] if with_pos else (refs[-1], None)
    part_refs, at = split_refs(refs, tails_count, parts)
    mp = lax.axis_index("mp")
    tails = [r[cap : cap + META, 0:LANES] for r in refs[:tails_count]]
    where_all = places(tails, cap)
    bits = [window_bits(tails[i]) for i in names]
    slot = lax.broadcasted_iota(jnp.int32, (WLEN, cap), 0)
    for i, p in enumerate(where_all if with_pos else []):
        pos_ref[i * cap : (i + 1) * cap, :] = jnp.transpose(
            jnp.broadcast_to(p.astype(F32), (LANES, cap))
        ).astype(jnp.int32)

    @pl.loop(0, table.shape[0] // WLEN)
    def _(w):
        at_rows = pl.ds(pl.multiple_of(w * WLEN, WLEN), WLEN)
        rows = table.at[at_rows, :]
        rows[...] = refs[at][at_rows, :] if has_prev else jnp.zeros(rows.shape, BF16)
        for i, name in enumerate(names):

            @pl.when((bits[i] >> w) & 1 == 1)
            def _():
                hot = (slot + w * WLEN == where_all[name]).astype(F32).astype(BF16)
                add_rows(rows, hot, part_refs[i], mp, mp_steps, piece, cap)


def project_kernel(*refs, names, parts, cap, mp_steps, tails_count, piece, local, sub_size, group):
    qkv_ref, weight_ref, member_ref = refs[-3:]
    part_refs, at = split_refs(refs, tails_count, parts)
    table_ref, wqk_ref, wv_ref, counts_ref = refs[at : at + 4]
    mp = lax.axis_index("mp")
    me = own_index(sub_size)
    tails = [r[cap : cap + META, 0:LANES] for r in refs[:tails_count]]
    where_all = places(tails, cap)
    bits = [window_bits(tails[i]) for i in names]
    for t in range(mp_steps.n):
        block = pl.ds(pl.multiple_of(mp_steps.frm(mp, t) * piece, piece), piece)
        to = slice(t * piece, (t + 1) * piece)
        weight_ref[to, 0:local] = wqk_ref[0, block, :]
        weight_ref[to, local : 2 * local] = wqk_ref[1, block, :]
        weight_ref[to, 2 * local : 3 * local] = wv_ref[block, :]
    slot = lax.broadcasted_iota(jnp.int32, (WLEN, cap), 0)
    windows = table_ref.shape[0] // WLEN

    @pl.loop(0, windows // group)
    def _(g):
        rows = pl.ds(pl.multiple_of(g * group * WLEN, WLEN), group * WLEN)
        live = counts_ref[me * windows + g * group]
        for j in range(1, group):
            live = live + counts_ref[me * windows + g * group + j]

        @pl.when(live > 0)
        def _():
            member_ref[...] = table_ref[rows, :]
            for j in range(group):
                w = g * group + j
                part_rows = member_ref.at[j * WLEN : (j + 1) * WLEN, :]
                for i, name in enumerate(names):

                    @pl.when((bits[i] >> w) & 1 == 1)
                    def _():
                        hot = (slot + w * WLEN == where_all[name]).astype(F32).astype(BF16)
                        add_rows(part_rows, hot, part_refs[i], mp, mp_steps, piece, cap)

            qkv_ref[rows, :] = dot(member_ref[...], weight_ref[...]).astype(BF16)


def attend_kernel(qkv_ref, counts_ref, att, *, pairs, local, sub_size, group):
    me = own_index(sub_size)
    windows = att.shape[0] // WLEN
    low = lax.broadcasted_iota(jnp.int32, (WLEN, LANES), 1) < HDIM
    key = lax.broadcasted_iota(jnp.int32, (1, WLEN), 1)
    factor = HDIM ** (-0.5) * 1.4426950408889634
    zero = jnp.zeros((WLEN, LANES), BF16)
    one = jnp.ones((WLEN, LANES), BF16)
    ones = [jnp.where(low, one, zero), jnp.where(low, zero, one)]

    def mix(rows, live):
        bias = jnp.where(key < live, 0.0, -1e30).astype(F32)
        for at, pair in enumerate(pairs):
            q = qkv_ref[rows, pair * LANES : (pair + 1) * LANES]
            k = qkv_ref[rows, local + pair * LANES : local + (pair + 1) * LANES]
            v = qkv_ref[rows, 2 * local + pair * LANES : 2 * local + (pair + 1) * LANES]
            both = jnp.concatenate([jnp.where(low, q, zero), jnp.where(low, zero, q)], axis=0)
            scores = lax.dot_general(both, k, (((1,), (1,)), ((), ())), preferred_element_type=F32)
            scores = scores + bias
            top = jnp.max(scores, axis=1, keepdims=True)
            grown = jnp.exp2((scores - top) * factor).astype(BF16)
            wide = jnp.concatenate([grown[:WLEN], grown[WLEN:]], axis=1)
            mixer = jnp.concatenate(
                [
                    jnp.concatenate([jnp.where(low, v, zero), ones[0]], axis=1),
                    jnp.concatenate([jnp.where(low, zero, v), ones[1]], axis=1),
                ],
                axis=0,
            )
            mixed = dot(wide, mixer)
            att[rows, at * LANES : (at + 1) * LANES] = (
                mixed[:, :LANES] / mixed[:, LANES:]
            ).astype(BF16)

    @pl.loop(0, windows // group)
    def _(g):
        lives = [counts_ref[me * windows + g * group + j] for j in range(group)]
        spans = [
            pl.ds(pl.multiple_of((g * group + j) * WLEN, WLEN), WLEN) for j in range(group)
        ]

        @pl.when(sum(lives) == 0)
        def _():
            for rows in spans:
                att[rows, :] = jnp.zeros((WLEN, att.shape[1]), BF16)

        @pl.when(sum(lives) > 0)
        def _():
            for rows, live in zip(spans, lives):
                mix(rows, live)


def fetch_kernel(att_ref, pos_ref, *outs, names, cap):
    slots = att_ref.shape[0]
    for i, k in enumerate(names):
        pos = pos_ref[k * cap : (k + 1) * cap, :]
        lane = lax.broadcasted_iota(jnp.int32, (cap, LANES), 1)
        hot = jnp.concatenate(
            [(pos == lane + t * LANES).astype(F32).astype(BF16) for t in range(slots // LANES)],
            axis=1,
        )
        outs[i][...] = dot(hot, att_ref[...]).astype(BF16)


def spots(dest, lane, base, cap):
    tiles = []
    for t in range(-(-cap // LANES)):
        tiles.append((dest == lane + (base + t * LANES)).astype(F32).astype(BF16))
    hot = tiles[0] if len(tiles) == 1 else jnp.concatenate(tiles, axis=1)
    return hot[:, 0:cap]


def unpack_kernel(*refs, names, cap, parts, local, block_rows):
    col_ref, out_ref = refs[-2], refs[-1]
    lane = lax.broadcasted_iota(jnp.int32, (block_rows, LANES), 1)

    @pl.loop(0, out_ref.shape[0] // block_rows)
    def _(b):
        rows = pl.ds(pl.multiple_of(b * block_rows, block_rows), block_rows)
        dest = col_ref[rows, :]
        heads = [None] * parts
        for i, k in enumerate(names):
            hot = spots(dest, lane, k * cap, cap)
            for t in range(parts):
                term = dot(hot, refs[i * parts + t][...])
                heads[t] = term if heads[t] is None else heads[t] + term
        for t in range(parts):
            out_ref[rows, t * local : (t + 1) * local] = heads[t].astype(BF16)


def final_kernel(*refs, names, cap, mp_steps, sub_size, local, block_rows):
    parts = mp_steps.n
    at = len(names) * parts
    early_ref, col_ref, vox_ref, gain_ref, wout_ref, wup_ref, wdown_ref = refs[at : at + 7]
    at += 7
    extra = refs[at : at + 3 * sub_size * (parts - 1)]
    out_ref, proj_ref = refs[-2], refs[-1]
    mp = lax.axis_index("mp")
    sub = lax.axis_index("sub")
    width = vox_ref.shape[1]
    out_width = out_ref.shape[1]
    mine = pl.ds(pl.multiple_of(mp * out_width, LANES), out_width)
    proj_ref[0:local, :] = wout_ref[...]
    ups, downs = [wup_ref], [None]
    part_rows = local // sub_size
    for t in range(1, parts):
        for j in range(sub_size):
            up, down, proj = extra[3 * ((t - 1) * sub_size + j) : 3 * ((t - 1) * sub_size + j) + 3]
            ups.append(up)
            downs.append(down)
            at_row = t * local + (sub + j) % sub_size * part_rows
            proj_ref[pl.ds(pl.multiple_of(at_row, part_rows), part_rows), :] = proj[...]
    lane = lax.broadcasted_iota(jnp.int32, (block_rows, LANES), 1)

    @pl.loop(0, vox_ref.shape[0] // block_rows)
    def _(b):
        rows = pl.ds(pl.multiple_of(b * block_rows, block_rows), block_rows)
        dest = col_ref[rows, :]
        heads = [early_ref[rows, t * local : (t + 1) * local].astype(F32) for t in range(parts)]
        for i, k in enumerate(names):
            hot = spots(dest, lane, k * cap, cap)
            for t in range(parts):
                heads[t] = heads[t] + dot(hot, refs[i * parts + t][...])
        every = jnp.concatenate([h.astype(BF16) for h in heads], axis=1)
        after = vox_ref[rows, :].astype(F32) + dot(every, proj_ref[...])
        normed = layer_norm(after, gain_ref[...]).astype(BF16)
        total = None
        for up, down in zip(ups, downs):
            u = dot(normed, up[...])
            inner = u * (0.7978845608028654 + (0.7978845608028654 * 0.044715) * (u * u))
            half = 0.5 * u
            hidden = (half + half * jnp.tanh(inner)).astype(BF16)
            term = dot(hidden, wdown_ref[:, mine] if down is None else down[...])
            total = term if total is None else total + term
        keep = after[:, 0:out_width]
        for j in range(1, width // out_width):
            keep = jnp.where(mp == j, after[:, j * out_width : (j + 1) * out_width], keep)
        out_ref[rows, :] = (keep + total).astype(BF16)


def far_order(n, near):
    if n == 8 and near == 2:
        return [4, 2, 5, 3, 6, 7]
    return list(range(near, n))


def near_count(n, sub_size):
    return sub_size if Steps(n).xor else 1


def shards(
    voxels, window_ids, voxel_slots, window_counts, norm_gain, w_query_key, w_value, w_out,
    ffn_gain, w_up, w_down, *, n, mp_size, sub_size,
):
    rows, width = voxels.shape
    cap = 2 * rows // n
    steps, mp_steps = Steps(n), Steps(mp_size)
    near = near_count(n, sub_size)
    far = far_order(n, near)
    order = list(range(near)) + far
    early, late = order[:-2], order[-2:]
    piece = width // mp_size
    local = w_value.shape[1]
    mp = lax.axis_index("mp")
    sub = lax.axis_index("sub")

    def over_mp(x, t):
        return lax.ppermute(x, "mp", mp_steps.perm(t))

    bucket = cap + META
    packed = pl.pallas_call(
        functools.partial(
            pack_kernel, steps=steps, sub_size=sub_size, near=near, cap=cap, wins=n * WIN_DEV
        ),
        out_shape=[jax.ShapeDtypeStruct((rows, LANES), jnp.int32)]
        + [jax.ShapeDtypeStruct((bucket, width if k < near else piece), BF16) for k in range(n)],
        in_specs=[VM, HB, HB],
        out_specs=[VM] * (n + 1),
        scratch_shapes=[
            pltpu.VMEM((rows, width), BF16), pltpu.VMEM((n * WIN_DEV, LANES), F32),
            pltpu.VMEM((rows, width), BF16), pltpu.VMEM((1, width), F32),
            pltpu.SemaphoreType.DMA, pltpu.SemaphoreType.DMA,
        ],
        compiler_params=PARAMS,
        name="pack",
    )(window_ids.reshape(1, rows), voxels, norm_gain.reshape(1, width))
    dest_col, packed = packed[0], packed[1:]

    part = w_up.shape[1] // sub_size
    out_part = w_out.shape[0] // sub_size
    pieces = []
    for t in range(1, mp_size):
        to = mp_steps.to(mp, t)
        pieces.append((
            lax.dynamic_slice_in_dim(w_up, sub * part, part, 1),
            lax.dynamic_slice(w_down, (sub * part, to * piece), (part, piece)),
            lax.dynamic_slice_in_dim(w_out, sub * out_part, out_part, 0),
        ))

    arrived = {0: [packed[0]]}
    for k in range(1, near):
        arrived[k] = [lax.ppermute(packed[k], OWN, steps.perm(k))]
    for i, k in enumerate(far):
        sent = packed[k]
        if i == 2:
            sent, pieces = lax.optimization_barrier((sent, pieces))
        got = lax.ppermute(sent, OWN, steps.perm(k))
        arrived[k] = [got] + [over_mp(got, t) for t in range(1, mp_size)]

    extra = []
    for t in range(1, mp_size):
        sent = [over_mp(x, t) for x in pieces[t - 1]]
        extra += sent
        for j in range(1, sub_size):
            share = [((i + j) % sub_size, i) for i in range(sub_size)]
            extra += [lax.ppermute(x, "sub", share) for x in sent]

    slots = WIN_DEV * WLEN
    tails = [arrived[k][0] for k in order]
    cuts = [0, min(near + 2, len(early)), len(early)]
    prev = []
    for number in range(2):
        group = list(range(cuts[number], cuts[number + 1]))
        parts = [arrived[order[i]] for i in group]
        with_pos = number == 1
        seen = tails if with_pos else tails[: cuts[1]]
        got = pl.pallas_call(
            functools.partial(
                place_kernel, names=group, parts=[len(p) for p in parts], cap=cap,
                mp_steps=mp_steps, tails_count=len(seen), piece=piece, has_prev=bool(prev),
                with_pos=with_pos,
            ),
            out_shape=[jax.ShapeDtypeStruct((slots, width), BF16)]
            + [jax.ShapeDtypeStruct((n * cap, LANES), jnp.int32)] * with_pos,
            in_specs=[VM] * (len(seen) + sum(len(p) for p in parts) + len(prev)),
            out_specs=[VM] * (1 + with_pos),
            compiler_params=PARAMS,
            name="place",
        )(*seen, *[x for p in parts for x in p], *prev)
        prev = [got[0]]
    table, pos = got
    flat = [x for k in late for x in arrived[k]]
    qkv = pl.pallas_call(
        functools.partial(
            project_kernel, names=[order.index(k) for k in late],
            parts=[len(arrived[k]) for k in late], cap=cap, mp_steps=mp_steps, tails_count=n,
            piece=piece, local=local, sub_size=sub_size, group=2,
        ),
        out_shape=jax.ShapeDtypeStruct((slots, 3 * local), BF16),
        in_specs=[VM] * (n + len(flat) + 3) + [SM],
        out_specs=VM,
        scratch_shapes=[pltpu.VMEM((width, 3 * local), BF16), pltpu.VMEM((2 * WLEN, width), BF16)],
        compiler_params=PARAMS,
        name="project",
    )(*tails, *flat, table, w_query_key, w_value, window_counts)
    att = pl.pallas_call(
        functools.partial(
            attend_kernel, pairs=list(range(local // LANES)), local=local, sub_size=sub_size,
            group=2,
        ),
        out_shape=jax.ShapeDtypeStruct((slots, local), BF16),
        in_specs=[VM, SM],
        out_specs=VM,
        compiler_params=PARAMS,
        name="attend",
    )(qkv, window_counts)

    answers = {}
    for group in (far[:2], list(range(near)) + far[2:]):
        got = pl.pallas_call(
            functools.partial(fetch_kernel, names=[order.index(k) for k in group], cap=cap),
            out_shape=[jax.ShapeDtypeStruct((cap, local), BF16) for _ in group],
            in_specs=[VM, VM],
            out_specs=[VM] * len(group),
            compiler_params=PARAMS,
            name="fetch",
        )(att, pos)
        answers.update(zip(group, got))
    returned = {}
    for k in order:
        home = answers[k]
        if k > 0:
            home = lax.ppermute(home, OWN, steps.perm(k, True))
        returned[k] = [home] + [over_mp(home, t) for t in range(1, mp_size)]

    block_rows = rows // 2
    flat = [x for k in early for x in returned[k]]
    heads = pl.pallas_call(
        functools.partial(
            unpack_kernel, names=early, cap=cap, parts=mp_size, local=local,
            block_rows=block_rows,
        ),
        out_shape=jax.ShapeDtypeStruct((rows, mp_size * local), BF16),
        in_specs=[VM] * (len(flat) + 1),
        out_specs=VM,
        compiler_params=PARAMS,
        name="unpack",
    )(*flat, dest_col)
    flat = [x for k in late for x in returned[k]]
    return pl.pallas_call(
        functools.partial(
            final_kernel, names=late, cap=cap, mp_steps=mp_steps, sub_size=sub_size, local=local,
            block_rows=block_rows,
        ),
        out_shape=jax.ShapeDtypeStruct((rows, piece), BF16),
        in_specs=[VM] * (len(flat) + 7 + len(extra)),
        out_specs=VM,
        scratch_shapes=[pltpu.VMEM((mp_size * local, width), BF16)],
        compiler_params=PARAMS,
        name="final",
    )(*flat, heads, dest_col, voxels, ffn_gain.reshape(1, width), w_out, w_up, w_down, *extra)


def solution(mesh):
    sizes = mesh.shape
    n, sub_size = sizes["space"] * sizes["sub"], sizes["sub"]

    def body(*args):
        return shards(*args, n=n, mp_size=sizes["mp"], sub_size=sub_size)

    return jax.shard_map(
        body,
        mesh=mesh,
        in_specs=(
            P(("groups", "space", "sub"), None),
            P(("groups", "space", "sub")),
            P(("groups", "space", "sub")),
            P("groups"),
            P(),
            P(None, None, "mp"),
            P(None, "mp"),
            P("mp", None),
            P(),
            P(None, "mp"),
            P("mp", None),
        ),
        out_specs=P(("groups", "space", "sub"), "mp"),
        check_vma=False,
    )
```

```python
import functools

import jax
import jax.numpy as jnp
from jax import lax
from jax.experimental import pallas as pl
from jax.experimental.pallas import tpu as pltpu
from jax.sharding import PartitionSpec as P


HDIM = 64
WLEN = 256
WIN_DEV = 16
META = 16
LANES = 128
OWN = ("space", "sub")
FIRST = 1
SLICES_AT = 4
FINAL_BLOCKS = 2


F32 = jnp.float32
BF16 = jnp.bfloat16
VM = pl.BlockSpec(memory_space=pltpu.VMEM)
SM = pl.BlockSpec(memory_space=pltpu.SMEM)
PARAMS = pltpu.CompilerParams(vmem_limit_bytes=20 * 1024 * 1024)


class Steps:
    def __init__(self, n):
        self.n = n
        self.xor = n & (n - 1) == 0

    def to(self, i, k):
        return i ^ k if self.xor else (i + k) % self.n

    def frm(self, i, k):
        return i ^ k if self.xor else (i + self.n - k) % self.n

    def step(self, i, owner):
        return owner ^ i if self.xor else (owner + self.n - i) % self.n

    def perm(self, k, back=False):
        go = self.frm if back else self.to
        return [(i, go(i, k)) for i in range(self.n)]


def layer_norm(values_in, gain):
    row_mean = jnp.mean(values_in, axis=-1, keepdims=True)
    centred = values_in - row_mean
    variance = jnp.mean(centred * centred, axis=-1, keepdims=True)
    return centred * lax.rsqrt(variance + 1e-05) * gain


def dot(a, b):
    return jnp.dot(a, b, preferred_element_type=F32)


def own_index(sub_size):
    return lax.axis_index("space") * sub_size + lax.axis_index("sub")


def pack_bucket(out, k, dest, row_iota, normed_ref, cnt_ref, me, mp, steps, near, cap):
    piece = out.shape[1]
    pick = (dest == row_iota + k * cap).astype(F32).astype(BF16)
    if k < near:
        source = normed_ref[...]
    else:
        source = normed_ref[:, pl.ds(pl.multiple_of(mp * piece, LANES), piece)]
    out[0:cap, :] = dot(pick, source).astype(BF16)
    at = pl.ds(pl.multiple_of(steps.to(me, k) * WIN_DEV, WIN_DEV), WIN_DEV)
    tail = cnt_ref[at, :]
    out[cap : cap + META, :] = jnp.concatenate([tail] * (piece // LANES), axis=1).astype(BF16)


def rank_kernel(ids_ref, dest_ref, cnt_ref, *, steps, sub_size, cap):
    wins = cnt_ref.shape[0]
    ids = ids_ref[...]
    rows = ids.shape[1]
    step = 256
    win_iota = lax.broadcasted_iota(jnp.int32, (wins, step), 0)
    upper = (
        lax.broadcasted_iota(jnp.int32, (step, step), 0)
        < lax.broadcasted_iota(jnp.int32, (step, step), 1)
    ).astype(F32).astype(BF16)
    hots, sums = [], []
    counts = jnp.zeros((wins, 1), F32)
    for b in range(rows // step):
        hot = (ids[:, b * step : (b + 1) * step] == win_iota).astype(F32)
        hots.append(hot)
        sums.append(jnp.sum(hot, axis=1, keepdims=True))
        counts = counts + sums[-1]
    wide = jnp.broadcast_to(counts, (wins, LANES))
    cnt_ref[...] = wide
    r_io = lax.broadcasted_iota(jnp.int32, (wins, wins), 0)
    c_io = lax.broadcasted_iota(jnp.int32, (wins, wins), 1)
    same = (r_io // WIN_DEV == c_io // WIN_DEV) & (c_io < r_io)
    carry = dot(same.astype(F32).astype(BF16), wide.astype(BF16))[:, :1]
    ranks = []
    for hot, total in zip(hots, sums):
        cum = dot(hot.astype(BF16), upper) + carry
        ranks.append(jnp.sum(hot * cum, axis=0, keepdims=True))
        carry = carry + total
    rank = jnp.concatenate(ranks, axis=1).astype(jnp.int32)
    dest_ref[...] = steps.step(own_index(sub_size), ids // WIN_DEV) * cap + rank


def pack_kernel(
    dest_ref, cnt_ref, vox_ref, gain_ref, normed_ref, *outs, steps, sub_size, near, cap, names
):
    rows = vox_ref.shape[0]
    me = own_index(sub_size)
    mp = lax.axis_index("mp")
    row_iota = lax.broadcasted_iota(jnp.int32, (cap, rows), 0)
    normed_ref[...] = layer_norm(vox_ref[...].astype(F32), gain_ref[...]).astype(BF16)
    for out, k in zip(outs, names):
        pack_bucket(
            out, k, dest_ref[...], row_iota, normed_ref, cnt_ref, me, mp, steps, near, cap
        )


def pack_rest_kernel(dest_ref, normed_ref, cnt_ref, col_ref, *outs, steps, sub_size, near, cap, names):
    rows = normed_ref.shape[0]
    me = own_index(sub_size)
    mp = lax.axis_index("mp")
    dest = dest_ref[...]
    row_iota = lax.broadcasted_iota(jnp.int32, (cap, rows), 0)
    for out, k in zip(outs, names):
        pack_bucket(out, k, dest, row_iota, normed_ref, cnt_ref, me, mp, steps, near, cap)
    col_ref[...] = jnp.transpose(jnp.broadcast_to(dest.astype(F32), (LANES, rows))).astype(jnp.int32)


def places(tails, cap):
    base = jnp.zeros((META, 1), F32)
    lower = (
        lax.broadcasted_iota(jnp.int32, (META, META), 1)
        < lax.broadcasted_iota(jnp.int32, (META, META), 0)
    ).astype(F32).astype(BF16)
    row = lax.broadcasted_iota(jnp.int32, (META, cap), 1).astype(F32)
    win = lax.broadcasted_iota(jnp.int32, (META, 1), 0).astype(F32) * WLEN
    out = []
    for tail in tails:
        start = dot(lower, tail)[:, :1]
        count = tail.astype(F32)[:, :1]
        inside = (row >= start) & (row < start + count)
        value = jnp.where(inside, win + base - start + row + 1.0, 0.0)
        out.append((jnp.sum(value, axis=0, keepdims=True) - 1.0).astype(jnp.int32))
        base = base + count
    return out


def window_bits(tail):
    power = jnp.left_shift(1, lax.broadcasted_iota(jnp.int32, (META, LANES), 0)).astype(F32)
    lane = lax.broadcasted_iota(jnp.int32, (META, LANES), 1)
    return jnp.sum(jnp.where((tail.astype(F32) > 0) & (lane == 0), power, 0.0)).astype(jnp.int32)


def split_refs(refs, at, parts):
    out = []
    for width in parts:
        out.append(refs[at : at + width])
        at += width
    return out, at


def add_rows(dest, hot, part, which, mp, mp_steps, piece, cap):
    for t, ref in zip(which, part if len(part) == len(which) else part * len(which)):
        if ref.shape[1] > piece:
            block = mp_steps.frm(mp, t)
            rows = ref[0:cap, pl.ds(pl.multiple_of(block * piece, LANES), piece)]
        else:
            rows = ref[0:cap, :]
        cols = slice(t * piece, (t + 1) * piece)
        dest[:, cols] = dest[:, cols] + dot(hot, rows).astype(BF16)


def weights_kernel(wqk_ref, wv_ref, out_ref, mp, mp_steps, piece):
    local = wv_ref.shape[1]
    for t in range(mp_steps.n):
        block = pl.ds(pl.multiple_of(mp_steps.frm(mp, t) * piece, piece), piece)
        to = slice(t * piece, (t + 1) * piece)
        out_ref[to, 0:local] = wqk_ref[0, block, :]
        out_ref[to, local : 2 * local] = wqk_ref[1, block, :]
        out_ref[to, 2 * local : 3 * local] = wv_ref[block, :]


def place_kernel(
    *refs, names, parts, which, cap, mp_steps, tails_count, piece, has_prev, weights
):
    table, side_ref = refs[-2:]
    part_refs, at = split_refs(refs, tails_count, parts)
    mp = lax.axis_index("mp")
    tails = [r[cap : cap + META, 0:LANES] for r in refs[:tails_count]]
    where_all = places(tails, cap)
    bits = [window_bits(tails[i]) for i in names]
    slot = lax.broadcasted_iota(jnp.int32, (WLEN, cap), 0)
    if weights:
        weights_kernel(*refs[at : at + 2], side_ref, mp, mp_steps, piece)
    for i, p in enumerate([] if weights else where_all):
        side_ref[i * cap : (i + 1) * cap, :] = jnp.transpose(
            jnp.broadcast_to(p.astype(F32), (LANES, cap))
        ).astype(jnp.int32)

    @pl.loop(0, table.shape[0] // WLEN)
    def _(w):
        at_rows = pl.ds(pl.multiple_of(w * WLEN, WLEN), WLEN)
        rows = table.at[at_rows, :]
        rows[...] = refs[at][at_rows, :] if has_prev else jnp.zeros(rows.shape, BF16)
        for i, name in enumerate(names):

            @pl.when((bits[i] >> w) & 1 == 1)
            def _():
                hot = (slot + w * WLEN == where_all[name]).astype(F32).astype(BF16)
                add_rows(rows, hot, part_refs[i], which[i], mp, mp_steps, piece, cap)


def project_kernel(
    *refs, names, parts, which, cap, mp_steps, tails_count, piece, sub_size, group
):
    qkv_ref, member_ref = refs[-2:]
    part_refs, at = split_refs(refs, tails_count, parts)
    table_ref, weight_ref, counts_ref = refs[at : at + 3]
    mp = lax.axis_index("mp")
    me = own_index(sub_size)
    tails = [r[cap : cap + META, 0:LANES] for r in refs[:tails_count]]
    where_all = places(tails, cap)
    bits = [window_bits(tails[i]) for i in names]
    slot = lax.broadcasted_iota(jnp.int32, (WLEN, cap), 0)
    windows = table_ref.shape[0] // WLEN

    @pl.loop(0, windows // group)
    def _(g):
        rows = pl.ds(pl.multiple_of(g * group * WLEN, WLEN), group * WLEN)
        live = counts_ref[me * windows + g * group]
        for j in range(1, group):
            live = live + counts_ref[me * windows + g * group + j]

        @pl.when(live > 0)
        def _():
            member_ref[...] = table_ref[rows, :]
            for j in range(group):
                w = g * group + j
                part_rows = member_ref.at[j * WLEN : (j + 1) * WLEN, :]
                for i, name in enumerate(names):

                    @pl.when((bits[i] >> w) & 1 == 1)
                    def _():
                        hot = (slot + w * WLEN == where_all[name]).astype(F32).astype(BF16)
                        add_rows(part_rows, hot, part_refs[i], which[i], mp, mp_steps, piece, cap)

            qkv_ref[rows, :] = dot(member_ref[...], weight_ref[...]).astype(BF16)


def attend_kernel(qkv_ref, counts_ref, att, *, pairs, local, sub_size, group):
    me = own_index(sub_size)
    windows = att.shape[0] // WLEN
    low = lax.broadcasted_iota(jnp.int32, (WLEN, LANES), 1) < HDIM
    key = lax.broadcasted_iota(jnp.int32, (1, WLEN), 1)
    factor = HDIM ** (-0.5) * 1.4426950408889634
    zero = jnp.zeros((WLEN, LANES), BF16)
    one = jnp.ones((WLEN, LANES), BF16)
    ones = [jnp.where(low, one, zero), jnp.where(low, zero, one)]

    def mix(rows, live):
        bias = jnp.where(key < live, 0.0, -1e30).astype(F32)
        for at, pair in enumerate(pairs):
            q = qkv_ref[rows, pair * LANES : (pair + 1) * LANES]
            k = qkv_ref[rows, local + pair * LANES : local + (pair + 1) * LANES]
            v = qkv_ref[rows, 2 * local + pair * LANES : 2 * local + (pair + 1) * LANES]
            both = jnp.concatenate([jnp.where(low, q, zero), jnp.where(low, zero, q)], axis=0)
            scores = lax.dot_general(both, k, (((1,), (1,)), ((), ())), preferred_element_type=F32)
            scores = scores + bias
            top = jnp.max(scores, axis=1, keepdims=True)
            grown = jnp.exp2((scores - top) * factor).astype(BF16)
            wide = jnp.concatenate([grown[:WLEN], grown[WLEN:]], axis=1)
            mixer = jnp.concatenate(
                [
                    jnp.concatenate([jnp.where(low, v, zero), ones[0]], axis=1),
                    jnp.concatenate([jnp.where(low, zero, v), ones[1]], axis=1),
                ],
                axis=0,
            )
            mixed = dot(wide, mixer)
            att[rows, at * LANES : (at + 1) * LANES] = (
                mixed[:, :LANES] / mixed[:, LANES:]
            ).astype(BF16)

    @pl.loop(0, windows // group)
    def _(g):
        lives = [counts_ref[me * windows + g * group + j] for j in range(group)]
        spans = [
            pl.ds(pl.multiple_of((g * group + j) * WLEN, WLEN), WLEN) for j in range(group)
        ]

        @pl.when(sum(lives) == 0)
        def _():
            for rows in spans:
                att[rows, :] = jnp.zeros((WLEN, att.shape[1]), BF16)

        @pl.when(sum(lives) > 0)
        def _():
            for rows, live in zip(spans, lives):
                mix(rows, live)


def fetch_kernel(att_ref, pos_ref, *outs, names, cap):
    slots = att_ref.shape[0]
    for i, k in enumerate(names):
        pos = pos_ref[k * cap : (k + 1) * cap, :]
        lane = lax.broadcasted_iota(jnp.int32, (cap, LANES), 1)
        hot = jnp.concatenate(
            [(pos == lane + t * LANES).astype(F32).astype(BF16) for t in range(slots // LANES)],
            axis=1,
        )
        outs[i][...] = dot(hot, att_ref[...]).astype(BF16)


def spots(dest, lane, base, cap):
    tiles = []
    for t in range(-(-cap // LANES)):
        tiles.append((dest == lane + (base + t * LANES)).astype(F32).astype(BF16))
    hot = tiles[0] if len(tiles) == 1 else jnp.concatenate(tiles, axis=1)
    return hot[:, 0:cap]


def unpack_kernel(*refs, items, cap, parts, local, block_rows):
    col_ref, out_ref = refs[-2], refs[-1]
    lane = lax.broadcasted_iota(jnp.int32, (block_rows, LANES), 1)

    @pl.loop(0, out_ref.shape[0] // block_rows)
    def _(b):
        rows = pl.ds(pl.multiple_of(b * block_rows, block_rows), block_rows)
        dest = col_ref[rows, :]
        heads = [None] * parts
        hots = {}
        for (k, t), ref in zip(items, refs):
            if k not in hots:
                hots[k] = spots(dest, lane, k * cap, cap)
            term = dot(hots[k], ref[...])
            heads[t] = term if heads[t] is None else heads[t] + term
        for t in range(parts):
            out_ref[rows, t * local : (t + 1) * local] = heads[t].astype(BF16)


def final_kernel(*refs, items, cap, mp_steps, sub_size, local, block_rows):
    parts = mp_steps.n
    at = len(items)
    early_ref, col_ref, vox_ref, gain_ref, wout_ref, wup_ref, wdown_ref = refs[at : at + 7]
    at += 7
    extra = refs[at : at + 3 * sub_size * (parts - 1)]
    out_ref, proj_ref = refs[-2:]
    mp = lax.axis_index("mp")
    sub = lax.axis_index("sub")
    width = vox_ref.shape[1]
    out_width = out_ref.shape[1]
    mine = pl.ds(pl.multiple_of(mp * out_width, LANES), out_width)
    proj_ref[0:local, :] = wout_ref[...]
    ups, downs = [wup_ref], [None]
    part_rows = local // sub_size
    for t in range(1, parts):
        for j in range(sub_size):
            up, down, proj = extra[3 * ((t - 1) * sub_size + j) : 3 * ((t - 1) * sub_size + j) + 3]
            ups.append(up)
            downs.append(down)
            at_row = t * local + (sub + j) % sub_size * part_rows
            proj_ref[pl.ds(pl.multiple_of(at_row, part_rows), part_rows), :] = proj[...]
    lane = lax.broadcasted_iota(jnp.int32, (block_rows, LANES), 1)

    @pl.loop(0, vox_ref.shape[0] // block_rows)
    def _(b):
        rows = pl.ds(pl.multiple_of(b * block_rows, block_rows), block_rows)
        dest = col_ref[rows, :]
        heads = [early_ref[rows, t * local : (t + 1) * local].astype(F32) for t in range(parts)]
        hots = {}
        for (k, t), ref in zip(items, refs):
            if k not in hots:
                hots[k] = spots(dest, lane, k * cap, cap)
            heads[t] = heads[t] + dot(hots[k], ref[...])
        every = jnp.concatenate([h.astype(BF16) for h in heads], axis=1)
        after = vox_ref[rows, :].astype(F32) + dot(every, proj_ref[...])
        normed = layer_norm(after, gain_ref[...]).astype(BF16)
        total = None
        for up, down in zip(ups, downs):
            u = dot(normed, up[...])
            inner = u * (0.7978845608028654 + (0.7978845608028654 * 0.044715) * (u * u))
            half = 0.5 * u
            hidden = (half + half * jnp.tanh(inner)).astype(BF16)
            term = dot(hidden, wdown_ref[:, mine] if down is None else down[...])
            total = term if total is None else total + term
        keep = after[:, 0:out_width]
        for j in range(1, width // out_width):
            keep = jnp.where(mp == j, after[:, j * out_width : (j + 1) * out_width], keep)
        out_ref[rows, :] = (keep + total).astype(BF16)


def far_order(n, near):
    if n == 8 and near == 2:
        return [4, 2, 6, 5, 3, 7]
    return list(range(near, n))


def near_count(n, sub_size):
    return sub_size if Steps(n).xor else 1


def shards(
    voxels, window_ids, voxel_slots, window_counts, norm_gain, w_query_key, w_value, w_out,
    ffn_gain, w_up, w_down, *, n, mp_size, sub_size,
):
    rows, width = voxels.shape
    cap = 2 * rows // n
    steps, mp_steps = Steps(n), Steps(mp_size)
    near = near_count(n, sub_size)
    far = far_order(n, near)
    order = list(range(near)) + far
    piece = width // mp_size
    local = w_value.shape[1]
    mp = lax.axis_index("mp")
    sub = lax.axis_index("sub")

    def over_mp(x, t):
        return lax.ppermute(x, "mp", mp_steps.perm(t))

    bucket = cap + META

    def bucket_shape(k):
        return jax.ShapeDtypeStruct((bucket, width if k < near else piece), BF16)

    first, rest = far[:FIRST], far[FIRST:] + list(range(near))
    common = dict(steps=steps, sub_size=sub_size, near=near, cap=cap)
    dest, counts = pl.pallas_call(
        functools.partial(rank_kernel, steps=steps, sub_size=sub_size, cap=cap),
        out_shape=[
            jax.ShapeDtypeStruct((1, rows), jnp.int32),
            jax.ShapeDtypeStruct((n * WIN_DEV, LANES), F32),
        ],
        in_specs=[VM],
        out_specs=[VM, VM],
        compiler_params=PARAMS,
        name="rank",
    )(window_ids.reshape(1, rows))
    got = pl.pallas_call(
        functools.partial(pack_kernel, names=first, **common),
        out_shape=[jax.ShapeDtypeStruct((rows, width), BF16)] + [bucket_shape(k) for k in first],
        in_specs=[VM] * 4,
        out_specs=[VM] * (1 + len(first)),
        compiler_params=PARAMS,
        name="pack",
    )(dest, counts, voxels, norm_gain.reshape(1, width))
    normed = got[0]
    packed = dict(zip(first, got[1:]))
    got = pl.pallas_call(
        functools.partial(pack_rest_kernel, names=rest, **common),
        out_shape=[jax.ShapeDtypeStruct((rows, LANES), jnp.int32)]
        + [bucket_shape(k) for k in rest],
        in_specs=[VM] * 3,
        out_specs=[VM] * (1 + len(rest)),
        compiler_params=PARAMS,
        name="pack",
    )(dest, normed, counts)
    dest_col = got[0]
    packed.update(zip(rest, got[1:]))

    part = w_up.shape[1] // sub_size
    out_part = w_out.shape[0] // sub_size
    pieces = []
    for t in range(1, mp_size):
        to = mp_steps.to(mp, t)
        pieces.append((
            lax.dynamic_slice_in_dim(w_up, sub * part, part, 1),
            lax.dynamic_slice(w_down, (sub * part, to * piece), (part, piece)),
            lax.dynamic_slice_in_dim(w_out, sub * out_part, out_part, 0),
        ))

    arrived = {0: [packed[0]]}
    for k in range(1, near):
        arrived[k] = [lax.ppermute(packed[k], OWN, steps.perm(k))]
    for i, k in enumerate(far):
        sent = packed[k]
        if i == min(SLICES_AT, len(far) - 1):
            sent, pieces = lax.optimization_barrier((sent, pieces))
        got = lax.ppermute(sent, OWN, steps.perm(k))
        arrived[k] = [got] + [over_mp(got, t) for t in range(1, mp_size)]

    extra = []
    for t in range(1, mp_size):
        sent = [over_mp(x, t) for x in pieces[t - 1]]
        extra += sent
        for j in range(1, sub_size):
            share = [((i + j) % sub_size, i) for i in range(sub_size)]
            extra += [lax.ppermute(x, "sub", share) for x in sent]

    slots = WIN_DEV * WLEN
    tails = [arrived[k][0] for k in order]
    every = tuple(range(mp_size))
    cut = near + 2
    work = [
        [(i, every) for i in range(cut)],
        [(i, every) for i in range(cut, n - 1)] + [(n - 1, every[:1])],
        [(n - 1, every[1:])] * (mp_size > 1),
    ]

    def place_args(items):
        names, which = [i for i, _ in items], [w for _, w in items]
        parts = [
            arrived[order[i]] if i < near else [arrived[order[i]][t] for t in w] for i, w in items
        ]
        keys = dict(names=names, which=which, parts=[len(p) for p in parts])
        return keys, [x for p in parts for x in p]

    prev = []
    for number in range(2):
        keys, flat = place_args(work[number])
        seen, tail_args, side = tails, prev, jax.ShapeDtypeStruct((n * cap, LANES), jnp.int32)
        if number == 0:
            seen, tail_args = tails[:cut], [w_query_key, w_value]
            side = jax.ShapeDtypeStruct((width, 3 * local), BF16)
        got = pl.pallas_call(
            functools.partial(
                place_kernel, cap=cap, mp_steps=mp_steps, tails_count=len(seen), piece=piece,
                has_prev=number == 1, weights=number == 0, **keys,
            ),
            out_shape=[jax.ShapeDtypeStruct((slots, width), BF16), side],
            in_specs=[VM] * (len(seen) + len(flat) + len(tail_args)),
            out_specs=[VM, VM],
            compiler_params=PARAMS,
            name="place",
        )(*seen, *flat, *tail_args)
        if number == 0:
            weight = got[1]
        prev = [got[0]]
    table, pos = got
    keys, flat = place_args(work[2])
    qkv = pl.pallas_call(
        functools.partial(
            project_kernel, cap=cap, mp_steps=mp_steps, tails_count=n, piece=piece,
            sub_size=sub_size, group=2, **keys,
        ),
        out_shape=jax.ShapeDtypeStruct((slots, 3 * local), BF16),
        in_specs=[VM] * (n + len(flat) + 2) + [SM],
        out_specs=VM,
        scratch_shapes=[pltpu.VMEM((2 * WLEN, width), BF16)],
        compiler_params=PARAMS,
        name="project",
    )(*tails, *flat, table, weight, window_counts)
    att = pl.pallas_call(
        functools.partial(
            attend_kernel, pairs=list(range(local // LANES)), local=local, sub_size=sub_size,
            group=2,
        ),
        out_shape=jax.ShapeDtypeStruct((slots, local), BF16),
        in_specs=[VM, SM],
        out_specs=VM,
        compiler_params=PARAMS,
        name="attend",
    )(qkv, window_counts)

    answers = {}
    for group in (far[:FIRST], list(range(near)) + far[FIRST:]):
        got = pl.pallas_call(
            functools.partial(fetch_kernel, names=[order.index(k) for k in group], cap=cap),
            out_shape=[jax.ShapeDtypeStruct((cap, local), BF16) for _ in group],
            in_specs=[VM, VM],
            out_specs=[VM] * len(group),
            compiler_params=PARAMS,
            name="fetch",
        )(att, pos)
        answers.update(zip(group, got))
    returned = {}
    for k in order:
        home = answers[k]
        if k > 0:
            home = lax.ppermute(home, OWN, steps.perm(k, True))
        returned[k] = [home] + [over_mp(home, t) for t in range(1, mp_size)]

    pieces_back = [(k, t) for k in order for t in every]
    soon = [x for x in pieces_back if x[0] not in order[-2:] or x[1] == 0]
    last = [x for x in pieces_back if x not in soon]
    heads = pl.pallas_call(
        functools.partial(
            unpack_kernel, items=soon, cap=cap, parts=mp_size, local=local,
            block_rows=rows // 2,
        ),
        out_shape=jax.ShapeDtypeStruct((rows, mp_size * local), BF16),
        in_specs=[VM] * (len(soon) + 1),
        out_specs=VM,
        compiler_params=PARAMS,
        name="unpack",
    )(*[returned[k][t] for k, t in soon], dest_col)
    flat = [returned[k][t] for k, t in last]
    return pl.pallas_call(
        functools.partial(
            final_kernel, items=last, cap=cap, mp_steps=mp_steps, sub_size=sub_size, local=local,
            block_rows=rows // FINAL_BLOCKS,
        ),
        out_shape=jax.ShapeDtypeStruct((rows, piece), BF16),
        in_specs=[VM] * (len(flat) + 7 + len(extra)),
        out_specs=VM,
        scratch_shapes=[pltpu.VMEM((mp_size * local, width), BF16)],
        compiler_params=PARAMS,
        name="final",
    )(*flat, heads, dest_col, voxels, ffn_gain.reshape(1, width), w_out, w_up, w_down, *extra)


def solution(mesh):
    sizes = mesh.shape
    n, sub_size = sizes["space"] * sizes["sub"], sizes["sub"]

    def body(*args):
        return shards(*args, n=n, mp_size=sizes["mp"], sub_size=sub_size)

    return jax.shard_map(
        body,
        mesh=mesh,
        in_specs=(
            P(("groups", "space", "sub"), None),
            P(("groups", "space", "sub")),
            P(("groups", "space", "sub")),
            P("groups"),
            P(),
            P(None, None, "mp"),
            P(None, "mp"),
            P("mp", None),
            P(),
            P(None, "mp"),
            P("mp", None),
        ),
        out_specs=P(("groups", "space", "sub"), "mp"),
        check_vma=False,
    )
```

```python
import functools

import jax
import jax.numpy as jnp
from jax import lax
from jax.experimental import pallas as pl
from jax.experimental.pallas import tpu as pltpu
from jax.sharding import PartitionSpec as P


HDIM = 64
WLEN = 256
WIN_DEV = 16
META = 16
LANES = 128
OWN = ("space", "sub")
FIRST = 1
SLICES_AT = 4
FINAL_BLOCKS = 2


F32 = jnp.float32
BF16 = jnp.bfloat16
VM = pl.BlockSpec(memory_space=pltpu.VMEM)
SM = pl.BlockSpec(memory_space=pltpu.SMEM)
PARAMS = pltpu.CompilerParams(vmem_limit_bytes=20 * 1024 * 1024)
PACKED = pltpu.CompilerParams(vmem_limit_bytes=20 * 1024 * 1024)


class Steps:
    def __init__(self, n):
        self.n = n
        self.xor = n & (n - 1) == 0

    def to(self, i, k):
        return i ^ k if self.xor else (i + k) % self.n

    def frm(self, i, k):
        return i ^ k if self.xor else (i + self.n - k) % self.n

    def step(self, i, owner):
        return owner ^ i if self.xor else (owner + self.n - i) % self.n

    def perm(self, k, back=False):
        go = self.frm if back else self.to
        return [(i, go(i, k)) for i in range(self.n)]


def layer_norm(values_in, gain):
    row_mean = jnp.mean(values_in, axis=-1, keepdims=True)
    centred = values_in - row_mean
    variance = jnp.mean(centred * centred, axis=-1, keepdims=True)
    return centred * lax.rsqrt(variance + 1e-05) * gain


def dot(a, b):
    return jnp.dot(a, b, preferred_element_type=F32)


def own_index(sub_size):
    return lax.axis_index("space") * sub_size + lax.axis_index("sub")


def pack_bucket(out, k, dest, row_iota, normed_ref, cnt_ref, me, mp, steps, near, cap):
    piece = out.shape[1]
    pick = (dest == row_iota + k * cap).astype(F32).astype(BF16)
    if k < near:
        source = normed_ref[...]
    else:
        source = normed_ref[:, pl.ds(pl.multiple_of(mp * piece, LANES), piece)]
    out[0:cap, :] = dot(pick, source).astype(BF16)
    at = pl.ds(pl.multiple_of(steps.to(me, k) * WIN_DEV, WIN_DEV), WIN_DEV)
    tail = cnt_ref[at, :]
    out[cap : cap + META, :] = jnp.concatenate([tail] * (piece // LANES), axis=1).astype(BF16)


def rank_kernel(ids_ref, dest_ref, cnt_ref, *, steps, sub_size, cap):
    wins = cnt_ref.shape[0]
    ids = ids_ref[...]
    rows = ids.shape[1]
    step = 256
    win_iota = lax.broadcasted_iota(jnp.int32, (wins, step), 0)
    upper = (
        lax.broadcasted_iota(jnp.int32, (step, step), 0)
        < lax.broadcasted_iota(jnp.int32, (step, step), 1)
    ).astype(F32).astype(BF16)
    hots, sums = [], []
    counts = jnp.zeros((wins, 1), F32)
    for b in range(rows // step):
        hot = (ids[:, b * step : (b + 1) * step] == win_iota).astype(F32)
        hots.append(hot)
        sums.append(jnp.sum(hot, axis=1, keepdims=True))
        counts = counts + sums[-1]
    wide = jnp.broadcast_to(counts, (wins, LANES))
    cnt_ref[...] = wide
    r_io = lax.broadcasted_iota(jnp.int32, (wins, wins), 0)
    c_io = lax.broadcasted_iota(jnp.int32, (wins, wins), 1)
    same = (r_io // WIN_DEV == c_io // WIN_DEV) & (c_io < r_io)
    carry = dot(same.astype(F32).astype(BF16), wide.astype(BF16))[:, :1]
    ranks = []
    for hot, total in zip(hots, sums):
        cum = dot(hot.astype(BF16), upper) + carry
        ranks.append(jnp.sum(hot * cum, axis=0, keepdims=True))
        carry = carry + total
    rank = jnp.concatenate(ranks, axis=1).astype(jnp.int32)
    dest_ref[...] = steps.step(own_index(sub_size), ids // WIN_DEV) * cap + rank


def pack_kernel(
    dest_ref, cnt_ref, vox_ref, gain_ref, normed_ref, *outs, steps, sub_size, near, cap, names
):
    rows = vox_ref.shape[0]
    me = own_index(sub_size)
    mp = lax.axis_index("mp")
    row_iota = lax.broadcasted_iota(jnp.int32, (cap, rows), 0)
    normed_ref[...] = layer_norm(vox_ref[...].astype(F32), gain_ref[...]).astype(BF16)
    for out, k in zip(outs, names):
        pack_bucket(
            out, k, dest_ref[...], row_iota, normed_ref, cnt_ref, me, mp, steps, near, cap
        )


def pack_rest_kernel(dest_ref, normed_ref, cnt_ref, col_ref, *outs, steps, sub_size, near, cap, names):
    rows = normed_ref.shape[0]
    me = own_index(sub_size)
    mp = lax.axis_index("mp")
    dest = dest_ref[...]
    row_iota = lax.broadcasted_iota(jnp.int32, (cap, rows), 0)
    for out, k in zip(outs, names):
        pack_bucket(out, k, dest, row_iota, normed_ref, cnt_ref, me, mp, steps, near, cap)
    col_ref[...] = jnp.transpose(jnp.broadcast_to(dest.astype(F32), (LANES, rows))).astype(jnp.int32)


def places(tails, cap):
    base = jnp.zeros((META, 1), F32)
    lower = (
        lax.broadcasted_iota(jnp.int32, (META, META), 1)
        < lax.broadcasted_iota(jnp.int32, (META, META), 0)
    ).astype(F32).astype(BF16)
    row = lax.broadcasted_iota(jnp.int32, (META, cap), 1).astype(F32)
    win = lax.broadcasted_iota(jnp.int32, (META, 1), 0).astype(F32) * WLEN
    out = []
    for tail in tails:
        start = dot(lower, tail)[:, :1]
        count = tail.astype(F32)[:, :1]
        inside = (row >= start) & (row < start + count)
        value = jnp.where(inside, win + base - start + row + 1.0, 0.0)
        out.append((jnp.sum(value, axis=0, keepdims=True) - 1.0).astype(jnp.int32))
        base = base + count
    return out


def window_bits(tail):
    power = jnp.left_shift(1, lax.broadcasted_iota(jnp.int32, (META, LANES), 0)).astype(F32)
    lane = lax.broadcasted_iota(jnp.int32, (META, LANES), 1)
    return jnp.sum(jnp.where((tail.astype(F32) > 0) & (lane == 0), power, 0.0)).astype(jnp.int32)


def split_refs(refs, at, parts):
    out = []
    for width in parts:
        out.append(refs[at : at + width])
        at += width
    return out, at


def add_rows(dest, hot, part, which, mp, mp_steps, piece, cap):
    for t, ref in zip(which, part if len(part) == len(which) else part * len(which)):
        if ref.shape[1] > piece:
            block = mp_steps.frm(mp, t)
            rows = ref[0:cap, pl.ds(pl.multiple_of(block * piece, LANES), piece)]
        else:
            rows = ref[0:cap, :]
        cols = slice(t * piece, (t + 1) * piece)
        dest[:, cols] = dest[:, cols] + dot(hot, rows).astype(BF16)


def weights_kernel(wqk_ref, wv_ref, out_ref, mp, mp_steps, piece):
    local = wv_ref.shape[1]
    for t in range(mp_steps.n):
        block = pl.ds(pl.multiple_of(mp_steps.frm(mp, t) * piece, piece), piece)
        to = slice(t * piece, (t + 1) * piece)
        out_ref[to, 0:local] = wqk_ref[0, block, :]
        out_ref[to, local : 2 * local] = wqk_ref[1, block, :]
        out_ref[to, 2 * local : 3 * local] = wv_ref[block, :]


def place_kernel(
    *refs, names, parts, which, cap, mp_steps, tails_count, piece, has_prev, weights
):
    table, side_ref = refs[-2:]
    part_refs, at = split_refs(refs, tails_count, parts)
    mp = lax.axis_index("mp")
    tails = [r[cap : cap + META, 0:LANES] for r in refs[:tails_count]]
    where_all = places(tails, cap)
    bits = [window_bits(tails[i]) for i in names]
    slot = lax.broadcasted_iota(jnp.int32, (WLEN, cap), 0)
    if weights:
        weights_kernel(*refs[at : at + 2], side_ref, mp, mp_steps, piece)
    for i, p in enumerate([] if weights else where_all):
        side_ref[i * cap : (i + 1) * cap, :] = jnp.transpose(
            jnp.broadcast_to(p.astype(F32), (LANES, cap))
        ).astype(jnp.int32)

    @pl.loop(0, table.shape[0] // WLEN)
    def _(w):
        at_rows = pl.ds(pl.multiple_of(w * WLEN, WLEN), WLEN)
        rows = table.at[at_rows, :]
        rows[...] = refs[at][at_rows, :] if has_prev else jnp.zeros(rows.shape, BF16)
        for i, name in enumerate(names):

            @pl.when((bits[i] >> w) & 1 == 1)
            def _():
                hot = (slot + w * WLEN == where_all[name]).astype(F32).astype(BF16)
                add_rows(rows, hot, part_refs[i], which[i], mp, mp_steps, piece, cap)


def project_kernel(
    *refs, names, parts, which, cap, mp_steps, tails_count, piece, sub_size, group
):
    qkv_ref, member_ref = refs[-2:]
    part_refs, at = split_refs(refs, tails_count, parts)
    table_ref, weight_ref, counts_ref = refs[at : at + 3]
    mp = lax.axis_index("mp")
    me = own_index(sub_size)
    tails = [r[cap : cap + META, 0:LANES] for r in refs[:tails_count]]
    where_all = places(tails, cap)
    bits = [window_bits(tails[i]) for i in names]
    slot = lax.broadcasted_iota(jnp.int32, (WLEN, cap), 0)
    windows = table_ref.shape[0] // WLEN

    @pl.loop(0, windows // group)
    def _(g):
        rows = pl.ds(pl.multiple_of(g * group * WLEN, WLEN), group * WLEN)
        live = counts_ref[me * windows + g * group]
        for j in range(1, group):
            live = live + counts_ref[me * windows + g * group + j]

        @pl.when(live > 0)
        def _():
            member_ref[...] = table_ref[rows, :]
            for j in range(group):
                w = g * group + j
                part_rows = member_ref.at[j * WLEN : (j + 1) * WLEN, :]
                for i, name in enumerate(names):

                    @pl.when((bits[i] >> w) & 1 == 1)
                    def _():
                        hot = (slot + w * WLEN == where_all[name]).astype(F32).astype(BF16)
                        add_rows(part_rows, hot, part_refs[i], which[i], mp, mp_steps, piece, cap)

            qkv_ref[rows, :] = dot(member_ref[...], weight_ref[...]).astype(BF16)


def attend_kernel(qkv_ref, counts_ref, att, *, pairs, local, sub_size, group):
    me = own_index(sub_size)
    windows = att.shape[0] // WLEN
    low = lax.broadcasted_iota(jnp.int32, (WLEN, LANES), 1) < HDIM
    key = lax.broadcasted_iota(jnp.int32, (1, WLEN), 1)
    factor = HDIM ** (-0.5) * 1.4426950408889634
    zero = jnp.zeros((WLEN, LANES), BF16)
    one = jnp.ones((WLEN, LANES), BF16)
    ones = [jnp.where(low, one, zero), jnp.where(low, zero, one)]

    def mix(rows, live):
        bias = jnp.where(key < live, 0.0, -1e30).astype(F32)
        for at, pair in enumerate(pairs):
            q = qkv_ref[rows, pair * LANES : (pair + 1) * LANES]
            k = qkv_ref[rows, local + pair * LANES : local + (pair + 1) * LANES]
            v = qkv_ref[rows, 2 * local + pair * LANES : 2 * local + (pair + 1) * LANES]
            both = jnp.concatenate([jnp.where(low, q, zero), jnp.where(low, zero, q)], axis=0)
            scores = lax.dot_general(both, k, (((1,), (1,)), ((), ())), preferred_element_type=F32)
            scores = scores + bias
            top = jnp.max(scores, axis=1, keepdims=True)
            grown = jnp.exp2((scores - top) * factor).astype(BF16)
            wide = jnp.concatenate([grown[:WLEN], grown[WLEN:]], axis=1)
            mixer = jnp.concatenate(
                [
                    jnp.concatenate([jnp.where(low, v, zero), ones[0]], axis=1),
                    jnp.concatenate([jnp.where(low, zero, v), ones[1]], axis=1),
                ],
                axis=0,
            )
            mixed = dot(wide, mixer)
            att[rows, at * LANES : (at + 1) * LANES] = (
                mixed[:, :LANES] / mixed[:, LANES:]
            ).astype(BF16)

    @pl.loop(0, windows // group)
    def _(g):
        lives = [counts_ref[me * windows + g * group + j] for j in range(group)]
        spans = [
            pl.ds(pl.multiple_of((g * group + j) * WLEN, WLEN), WLEN) for j in range(group)
        ]

        @pl.when(sum(lives) == 0)
        def _():
            for rows in spans:
                att[rows, :] = jnp.zeros((WLEN, att.shape[1]), BF16)

        @pl.when(sum(lives) > 0)
        def _():
            for rows, live in zip(spans, lives):
                mix(rows, live)


def fetch_kernel(att_ref, pos_ref, *outs, names, cap):
    slots = att_ref.shape[0]
    for i, k in enumerate(names):
        pos = pos_ref[k * cap : (k + 1) * cap, :]
        lane = lax.broadcasted_iota(jnp.int32, (cap, LANES), 1)
        hot = jnp.concatenate(
            [(pos == lane + t * LANES).astype(F32).astype(BF16) for t in range(slots // LANES)],
            axis=1,
        )
        outs[i][...] = dot(hot, att_ref[...]).astype(BF16)


def spots(dest, lane, base, cap):
    tiles = []
    for t in range(-(-cap // LANES)):
        tiles.append((dest == lane + (base + t * LANES)).astype(F32).astype(BF16))
    hot = tiles[0] if len(tiles) == 1 else jnp.concatenate(tiles, axis=1)
    return hot[:, 0:cap]


def unpack_kernel(*refs, items, cap, parts, local, block_rows):
    col_ref, out_ref = refs[-2], refs[-1]
    lane = lax.broadcasted_iota(jnp.int32, (block_rows, LANES), 1)

    @pl.loop(0, out_ref.shape[0] // block_rows)
    def _(b):
        rows = pl.ds(pl.multiple_of(b * block_rows, block_rows), block_rows)
        dest = col_ref[rows, :]
        heads = [None] * parts
        hots = {}
        for (k, t), ref in zip(items, refs):
            if k not in hots:
                hots[k] = spots(dest, lane, k * cap, cap)
            term = dot(hots[k], ref[...])
            heads[t] = term if heads[t] is None else heads[t] + term
        for t in range(parts):
            out_ref[rows, t * local : (t + 1) * local] = heads[t].astype(BF16)


def final_kernel(*refs, items, cap, mp_steps, sub_size, local, block_rows):
    parts = mp_steps.n
    at = len(items)
    early_ref, col_ref, vox_ref, gain_ref, wout_ref, wup_ref, wdown_ref = refs[at : at + 7]
    at += 7
    extra = refs[at : at + 3 * sub_size * (parts - 1)]
    out_ref, proj_ref = refs[-2:]
    mp = lax.axis_index("mp")
    sub = lax.axis_index("sub")
    width = vox_ref.shape[1]
    out_width = out_ref.shape[1]
    mine = pl.ds(pl.multiple_of(mp * out_width, LANES), out_width)
    proj_ref[0:local, :] = wout_ref[...]
    ups, downs = [wup_ref], [None]
    part_rows = local // sub_size
    for t in range(1, parts):
        for j in range(sub_size):
            up, down, proj = extra[3 * ((t - 1) * sub_size + j) : 3 * ((t - 1) * sub_size + j) + 3]
            ups.append(up)
            downs.append(down)
            at_row = t * local + (sub + j) % sub_size * part_rows
            proj_ref[pl.ds(pl.multiple_of(at_row, part_rows), part_rows), :] = proj[...]
    lane = lax.broadcasted_iota(jnp.int32, (block_rows, LANES), 1)

    @pl.loop(0, vox_ref.shape[0] // block_rows)
    def _(b):
        rows = pl.ds(pl.multiple_of(b * block_rows, block_rows), block_rows)
        dest = col_ref[rows, :]
        heads = [early_ref[rows, t * local : (t + 1) * local].astype(F32) for t in range(parts)]
        hots = {}
        for (k, t), ref in zip(items, refs):
            if k not in hots:
                hots[k] = spots(dest, lane, k * cap, cap)
            heads[t] = heads[t] + dot(hots[k], ref[...])
        every = jnp.concatenate([h.astype(BF16) for h in heads], axis=1)
        after = vox_ref[rows, :].astype(F32) + dot(every, proj_ref[...])
        normed = layer_norm(after, gain_ref[...]).astype(BF16)
        total = None
        for up, down in zip(ups, downs):
            u = dot(normed, up[...])
            inner = u * (0.7978845608028654 + (0.7978845608028654 * 0.044715) * (u * u))
            half = 0.5 * u
            hidden = (half + half * jnp.tanh(inner)).astype(BF16)
            term = dot(hidden, wdown_ref[:, mine] if down is None else down[...])
            total = term if total is None else total + term
        keep = after[:, 0:out_width]
        for j in range(1, width // out_width):
            keep = jnp.where(mp == j, after[:, j * out_width : (j + 1) * out_width], keep)
        out_ref[rows, :] = (keep + total).astype(BF16)


def far_order(n, near):
    if n == 8 and near == 2:
        return [4, 2, 6, 5, 3, 7]
    return list(range(near, n))


def near_count(n, sub_size):
    return sub_size if Steps(n).xor else 1


def shards(
    voxels, window_ids, voxel_slots, window_counts, norm_gain, w_query_key, w_value, w_out,
    ffn_gain, w_up, w_down, *, n, mp_size, sub_size,
):
    rows, width = voxels.shape
    cap = 2 * rows // n
    steps, mp_steps = Steps(n), Steps(mp_size)
    near = near_count(n, sub_size)
    far = far_order(n, near)
    order = list(range(near)) + far
    piece = width // mp_size
    local = w_value.shape[1]
    mp = lax.axis_index("mp")
    sub = lax.axis_index("sub")

    def over_mp(x, t):
        return lax.ppermute(x, "mp", mp_steps.perm(t))

    bucket = cap + META

    def bucket_shape(k):
        return jax.ShapeDtypeStruct((bucket, width if k < near else piece), BF16)

    first, rest = far[:FIRST], far[FIRST:] + list(range(near))
    common = dict(steps=steps, sub_size=sub_size, near=near, cap=cap)
    dest, counts = pl.pallas_call(
        functools.partial(rank_kernel, steps=steps, sub_size=sub_size, cap=cap),
        out_shape=[
            jax.ShapeDtypeStruct((1, rows), jnp.int32),
            jax.ShapeDtypeStruct((n * WIN_DEV, LANES), F32),
        ],
        in_specs=[VM],
        out_specs=[VM, VM],
        compiler_params=PARAMS,
        name="rank",
    )(window_ids.reshape(1, rows))
    got = pl.pallas_call(
        functools.partial(pack_kernel, names=first, **common),
        out_shape=[jax.ShapeDtypeStruct((rows, width), BF16)] + [bucket_shape(k) for k in first],
        in_specs=[VM] * 4,
        out_specs=[VM] * (1 + len(first)),
        compiler_params=PARAMS,
        name="pack",
    )(dest, counts, voxels, norm_gain.reshape(1, width))
    normed = got[0]
    packed = dict(zip(first, got[1:]))
    got = pl.pallas_call(
        functools.partial(pack_rest_kernel, names=rest, **common),
        out_shape=[jax.ShapeDtypeStruct((rows, LANES), jnp.int32)]
        + [bucket_shape(k) for k in rest],
        in_specs=[VM] * 3,
        out_specs=[VM] * (1 + len(rest)),
        compiler_params=PARAMS,
        name="pack",
    )(dest, normed, counts)
    dest_col = got[0]
    packed.update(zip(rest, got[1:]))

    part = w_up.shape[1] // sub_size
    out_part = w_out.shape[0] // sub_size
    pieces = []
    for t in range(1, mp_size):
        to = mp_steps.to(mp, t)
        pieces.append((
            lax.dynamic_slice_in_dim(w_up, sub * part, part, 1),
            lax.dynamic_slice(w_down, (sub * part, to * piece), (part, piece)),
            lax.dynamic_slice_in_dim(w_out, sub * out_part, out_part, 0),
        ))

    arrived = {0: [packed[0]]}
    for k in range(1, near):
        arrived[k] = [lax.ppermute(packed[k], OWN, steps.perm(k))]
    for i, k in enumerate(far):
        sent = packed[k]
        if i == min(SLICES_AT, len(far) - 1):
            sent, pieces = lax.optimization_barrier((sent, pieces))
        got = lax.ppermute(sent, OWN, steps.perm(k))
        arrived[k] = [got] + [over_mp(got, t) for t in range(1, mp_size)]

    extra = []
    for t in range(1, mp_size):
        sent = [over_mp(x, t) for x in pieces[t - 1]]
        extra += sent
        for j in range(1, sub_size):
            share = [((i + j) % sub_size, i) for i in range(sub_size)]
            extra += [lax.ppermute(x, "sub", share) for x in sent]

    slots = WIN_DEV * WLEN
    tails = [arrived[k][0] for k in order]
    every = tuple(range(mp_size))
    cut = near + 2
    work = [
        [(i, every) for i in range(cut)],
        [(i, every) for i in range(cut, n - 1)] + [(n - 1, every[:1])],
        [(n - 1, every[1:])] * (mp_size > 1),
    ]

    def place_args(items):
        names, which = [i for i, _ in items], [w for _, w in items]
        parts = [
            arrived[order[i]] if i < near else [arrived[order[i]][t] for t in w] for i, w in items
        ]
        keys = dict(names=names, which=which, parts=[len(p) for p in parts])
        return keys, [x for p in parts for x in p]

    prev = []
    for number in range(2):
        keys, flat = place_args(work[number])
        seen, tail_args, side = tails, prev, jax.ShapeDtypeStruct((n * cap, LANES), jnp.int32)
        if number == 0:
            seen, tail_args = tails[:cut], [w_query_key, w_value]
            side = jax.ShapeDtypeStruct((width, 3 * local), BF16)
        got = pl.pallas_call(
            functools.partial(
                place_kernel, cap=cap, mp_steps=mp_steps, tails_count=len(seen), piece=piece,
                has_prev=number == 1, weights=number == 0, **keys,
            ),
            out_shape=[jax.ShapeDtypeStruct((slots, width), BF16), side],
            in_specs=[VM] * (len(seen) + len(flat) + len(tail_args)),
            out_specs=[VM, VM],
            compiler_params=PARAMS,
            name="place",
        )(*seen, *flat, *tail_args)
        if number == 0:
            weight = got[1]
        prev = [got[0]]
    table, pos = got
    keys, flat = place_args(work[2])
    qkv = pl.pallas_call(
        functools.partial(
            project_kernel, cap=cap, mp_steps=mp_steps, tails_count=n, piece=piece,
            sub_size=sub_size, group=2, **keys,
        ),
        out_shape=jax.ShapeDtypeStruct((slots, 3 * local), BF16),
        in_specs=[VM] * (n + len(flat) + 2) + [SM],
        out_specs=VM,
        scratch_shapes=[pltpu.VMEM((2 * WLEN, width), BF16)],
        compiler_params=PARAMS,
        name="project",
    )(*tails, *flat, table, weight, window_counts)
    att = pl.pallas_call(
        functools.partial(
            attend_kernel, pairs=list(range(local // LANES)), local=local, sub_size=sub_size,
            group=2,
        ),
        out_shape=jax.ShapeDtypeStruct((slots, local), BF16),
        in_specs=[VM, SM],
        out_specs=VM,
        compiler_params=PACKED,
        name="attend",
    )(qkv, window_counts)

    answers = {}
    for group in (far[:FIRST], list(range(near)) + far[FIRST:]):
        got = pl.pallas_call(
            functools.partial(fetch_kernel, names=[order.index(k) for k in group], cap=cap),
            out_shape=[jax.ShapeDtypeStruct((cap, local), BF16) for _ in group],
            in_specs=[VM, VM],
            out_specs=[VM] * len(group),
            compiler_params=PARAMS,
            name="fetch",
        )(att, pos)
        answers.update(zip(group, got))
    returned = {}
    for k in order:
        home = answers[k]
        if k > 0:
            home = lax.ppermute(home, OWN, steps.perm(k, True))
        returned[k] = [home] + [over_mp(home, t) for t in range(1, mp_size)]

    pieces_back = [(k, t) for k in order for t in every]
    soon = [x for x in pieces_back if x[0] not in order[-2:] or x[1] == 0]
    last = [x for x in pieces_back if x not in soon]
    heads = pl.pallas_call(
        functools.partial(
            unpack_kernel, items=soon, cap=cap, parts=mp_size, local=local,
            block_rows=rows // 2,
        ),
        out_shape=jax.ShapeDtypeStruct((rows, mp_size * local), BF16),
        in_specs=[VM] * (len(soon) + 1),
        out_specs=VM,
        compiler_params=PARAMS,
        name="unpack",
    )(*[returned[k][t] for k, t in soon], dest_col)
    flat = [returned[k][t] for k, t in last]
    return pl.pallas_call(
        functools.partial(
            final_kernel, items=last, cap=cap, mp_steps=mp_steps, sub_size=sub_size, local=local,
            block_rows=rows // FINAL_BLOCKS,
        ),
        out_shape=jax.ShapeDtypeStruct((rows, piece), BF16),
        in_specs=[VM] * (len(flat) + 7 + len(extra)),
        out_specs=VM,
        scratch_shapes=[pltpu.VMEM((mp_size * local, width), BF16)],
        compiler_params=PACKED,
        name="final",
    )(*flat, heads, dest_col, voxels, ffn_gain.reshape(1, width), w_out, w_up, w_down, *extra)


def solution(mesh):
    sizes = mesh.shape
    n, sub_size = sizes["space"] * sizes["sub"], sizes["sub"]

    def body(*args):
        return shards(*args, n=n, mp_size=sizes["mp"], sub_size=sub_size)

    return jax.shard_map(
        body,
        mesh=mesh,
        in_specs=(
            P(("groups", "space", "sub"), None),
            P(("groups", "space", "sub")),
            P(("groups", "space", "sub")),
            P("groups"),
            P(),
            P(None, None, "mp"),
            P(None, "mp"),
            P("mp", None),
            P(),
            P(None, "mp"),
            P("mp", None),
        ),
        out_specs=P(("groups", "space", "sub"), "mp"),
        check_vma=False,
    )
```
